32 devices in a mesh: section: 4 (over z), tp: 8 (over y, x, core).
Axes of the slice: x: 2, y: 2, z: 4, core: 2. Of those that a mesh axis runs over, the one named last changes fastest.
Arguments:
- latents: bfloat16 [1024, 8, 2048], P('tp', 'section'), may hold values from -6 to 6
- timestep: int32 [8], replicated, may hold values from 0 to 999
- target: int32 [8], replicated, may hold values from 0 to 3, as said below
- qkv_weight: bfloat16 [4, 2048, 3, 2048], P('section', None, None, 'tp'), may hold values from -0.125 to 0.125
- mod_weight: bfloat16 [4, 256, 3, 2048], P('section'), may hold values from -2.6 to 2.6
- out_weight: bfloat16 [4, 2048, 2048], P('section', 'tp'), may hold values from -0.125 to 0.125
Outputs:
- updated: bfloat16 [1024, 8, 2048], P('tp', 'section')
The draws below stay inside these ranges and needn't reach their ends.
Inputs may be any that keep to these rules, and one draw needn't show every extreme that they name: target[l] is l // 2 or l // 2 + 1; of one section's 2 latents at most 1 name the next section, exactly 1 for section 0, none for the last section.
All inputs are finite; a program needn't handle non-finite values.
Results may differ from the reference program's by a relative error of at most 0.023.
Values may be sent and summed in bfloat16 or wider, within the bound.
A program may use at most 128 MiB of HBM per device.

```python
import math
import jax
import jax.numpy as jnp
from jax import lax

D = 2048
HEADS = 16
HEAD_DIM = 128
FREQ = 256
TOK = 1024
LAT_SECTION = 2
MOVE_MAX = 1
SECTIONS = 4
LATENTS = 8
N_TP = 8


def draw_target(key, part):
    counts = jax.random.randint(jax.random.fold_in(key, 11), (SECTIONS,), 0, MOVE_MAX + 1)
    section_ids = jnp.arange(SECTIONS, dtype=jnp.int32)
    counts = jnp.where(section_ids == 0, MOVE_MAX, counts)
    counts = jnp.where(section_ids == SECTIONS - 1, 0, counts)
    row_keys = jax.random.split(jax.random.fold_in(key, 12), SECTIONS)
    ranks = jax.vmap(lambda row_key: jax.random.permutation(row_key, LAT_SECTION))(row_keys)
    movers = (ranks < counts[:, None]).astype(jnp.int32)
    return (section_ids[:, None] + movers).reshape(LATENTS).astype(jnp.int32)


def draw_mod_weight(key, part):
    base = jnp.clip(jax.random.normal(jax.random.fold_in(key, 21), (SECTIONS, FREQ, 3, D), jnp.float32), -4.0, 4.0)
    return (base * 0.2).astype(jnp.bfloat16)


def with_ends(result, rng, low, largest):
    place = [jax.random.randint(jax.random.fold_in(rng, axis), (), 0, length) for axis, length in enumerate(result.shape)]
    main_axis = result.shape.index(max(result.shape))
    next_to = place[:main_axis] + [(place[main_axis] + 1) % result.shape[main_axis]] + place[main_axis + 1:]
    return result.at[tuple(place)].set(low).at[tuple(next_to)].set(largest)


def level_of(key, extent, cuts, low, high):
    def one(position, blocks):
        heights = jax.random.uniform(jax.random.fold_in(jax.random.fold_in(key, 6), position), (blocks,), jnp.float32, low / len(cuts), high / len(cuts))
        return jnp.repeat(jnp.exp(heights), extent[position] // blocks).reshape((-1,) + (1,) * (len(extent) - position - 1))

    gain = one(*cuts[0])
    for cut in cuts[1:]:
        gain = gain * one(*cut)
    return gain


def scatter_about(own_key, extent, spread, limit, pieces=(), kind=jnp.bfloat16):
    result = jax.random.normal(own_key, extent, jnp.float32) * spread
    if len(pieces) > 0:
        result = level_of(own_key, extent, pieces, -0.22, 0.18) * result
    return jnp.clip(result, min=-limit, max=limit).astype(kind)


def setup_inputs(seed: int = 0) -> dict:
    seeds = jax.random.split(jax.random.key(seed), 7)
    return {
        "latents": scatter_about(seeds[0], (TOK, LATENTS, D), 1.0, 6.0, ((0, 8), (1, 4))),
        "timestep": with_ends(jax.random.randint(seeds[1], (LATENTS,), 0, 1000), jax.random.fold_in(seeds[1], 1), 0, 999).astype(jnp.int32),
        "target": draw_target(jax.random.fold_in(seeds[6], 71), 0),
        "qkv_weight": scatter_about(seeds[3], (SECTIONS, D, 3, D), D ** -0.5, 0.125, ((0, 4), (3, 8))),
        "mod_weight": draw_mod_weight(jax.random.fold_in(seeds[6], 71), 0),
        "out_weight": scatter_about(seeds[5], (SECTIONS, D, D), D ** -0.5, 0.125, ((0, 4), (1, 8))),
    }


def time_embed(steps):
    half_width = FREQ // 2
    frequency = jnp.exp(-math.log(10000.0) * jnp.arange(half_width, dtype=jnp.float32) / half_width)
    angles = steps.astype(jnp.float32)[:, None] * frequency[None, :]
    return jnp.concatenate([jnp.cos(angles), jnp.sin(angles)], axis=1)

def modulate(steps, mod_table):
    feature = jax.nn.silu(time_embed(steps))
    return jnp.einsum('bf,fcd->bcd', feature, mod_table.astype(jnp.float32), precision=lax.Precision.HIGHEST)

def normalize(values, shift, scale):
    row_mean = lax.optimization_barrier(jnp.mean(values, axis=-1, keepdims=True))
    centred = values - row_mean
    variance = lax.optimization_barrier(jnp.mean(centred * centred, axis=-1, keepdims=True))
    return centred * lax.rsqrt(variance + 1e-06) * (1.0 + scale) + shift

def reference(latents, timestep, target, qkv_weight, mod_weight, out_weight):

    def one_latent(index):
        tokens = lax.dynamic_index_in_dim(latents, index, 1, keepdims=False)
        section_id = lax.dynamic_index_in_dim(target, index, 0, keepdims=False)
        step_now = lax.dynamic_slice_in_dim(timestep, index, 1)
        table = lax.dynamic_index_in_dim(mod_weight, section_id, 0, keepdims=False)
        qkv_table = lax.dynamic_index_in_dim(qkv_weight, section_id, 0, keepdims=False)
        out_table = lax.dynamic_index_in_dim(out_weight, section_id, 0, keepdims=False)
        mods = modulate(step_now, table)[0]
        values = tokens.astype(jnp.float32)
        hidden = normalize(values, mods[0], mods[1]).astype(jnp.bfloat16)
        packed = jnp.dot(hidden, qkv_table.reshape(D, 3 * D), preferred_element_type=jnp.float32)
        packed = packed.astype(jnp.bfloat16).reshape(TOK, 3, HEADS, HEAD_DIM)
        query = packed[:, 0].astype(jnp.float32)
        keys = packed[:, 1].astype(jnp.float32)
        vals = packed[:, 2].astype(jnp.float32)
        scores = jnp.einsum('qhe,khe->hqk', query, keys) * HEAD_DIM ** (-0.5)
        soft = jax.nn.softmax(scores, axis=-1).astype(jnp.bfloat16)
        mixed = jnp.einsum('hqk,khe->qhe', soft.astype(jnp.float32), vals).astype(jnp.bfloat16)
        grouped = mixed.reshape(TOK, N_TP, D // N_TP).astype(jnp.float32)
        out_groups = out_table.reshape(N_TP, D // N_TP, D).astype(jnp.float32)
        partial_terms = jnp.einsum('sgk,gkd->gsd', grouped, out_groups).astype(jnp.bfloat16)
        partial_terms = lax.optimization_barrier(partial_terms)
        proj = lax.optimization_barrier(jnp.sum(partial_terms.astype(jnp.float32), axis=0))
        return (values + mods[2] * proj).astype(jnp.bfloat16)
    results = lax.map(one_latent, jnp.arange(LATENTS, dtype=jnp.int32))
    return jnp.moveaxis(results, 0, 1)
```

```python
import functools
import math

import jax
import jax.numpy as jnp
from jax import lax
from jax.experimental import pallas as pl
from jax.experimental.pallas import tpu as pltpu
from jax.sharding import PartitionSpec as P

HEAD_DIM = 128
FREQ = 256
MOVE_MAX = 1


def from_behind(shard, axis, by):
    peers = lax.axis_size(axis)
    pairs = [(i, i + by) for i in range(peers) if 0 <= i + by < peers]
    return lax.ppermute(shard, axis, pairs)


def time_embed(steps):
    half_width = FREQ // 2
    frequency = jnp.exp(-math.log(10000.0) * jnp.arange(half_width, dtype=jnp.float32) / half_width)
    angles = steps.astype(jnp.float32)[:, None] * frequency[None, :]
    return jnp.concatenate([jnp.cos(angles), jnp.sin(angles)], axis=1)


def modulate(steps, mod_table):
    feature = jax.nn.silu(time_embed(steps))
    return jnp.einsum(
        "bf,fcd->bcd", feature, mod_table.astype(jnp.float32), precision=lax.Precision.HIGHEST
    )


def normalize(values, shift, scale):
    row_mean = jnp.mean(values, axis=-1, keepdims=True)
    centred = values - row_mean
    variance = jnp.mean(centred * centred, axis=-1, keepdims=True)
    return centred * lax.rsqrt(variance + 1e-06) * (1.0 + scale) + shift


def expert_block(batch, steps, qkv_local, mod_table, out_local):
    mods = modulate(steps, mod_table)
    values = batch.astype(jnp.float32)
    hidden = normalize(values, mods[None, :, 0], mods[None, :, 1]).astype(jnp.bfloat16)
    packed = jnp.einsum(
        "sbd,dce->sbce",
        lax.all_gather(hidden, "tp", axis=0, tiled=True),
        qkv_local,
        preferred_element_type=jnp.float32,
    ).astype(jnp.bfloat16)
    tok_all = packed.shape[0]
    slot_count = packed.shape[1]
    local_width = packed.shape[3]
    head_local = local_width // HEAD_DIM
    split_heads = packed.reshape(tok_all, slot_count, 3, head_local, HEAD_DIM)
    query = split_heads[:, :, 0]
    keys_now = split_heads[:, :, 1]
    vals_now = split_heads[:, :, 2]
    scores = jnp.einsum(
        "qbhe,kbhe->bhqk", query, keys_now, preferred_element_type=jnp.float32
    ) * HEAD_DIM ** (-0.5)
    soft = jax.nn.softmax(scores, axis=-1).astype(jnp.bfloat16)
    mixed = jnp.einsum("bhqk,kbhe->qbhe", soft, vals_now, preferred_element_type=jnp.float32)
    mixed = mixed.astype(jnp.bfloat16).reshape(tok_all, slot_count, local_width)
    proj = lax.psum_scatter(
        jnp.einsum("sbk,kd->sbd", mixed, out_local, preferred_element_type=jnp.float32).astype(
            jnp.bfloat16
        ),
        "tp",
        scatter_dimension=0,
        tiled=True,
    ).astype(jnp.float32)
    return (values + mods[None, :, 2] * proj).astype(jnp.bfloat16)


def movers_first(move_flags, slots):
    order_keys = jnp.where(move_flags, 0, 1).astype(jnp.int32) * slots + jnp.arange(
        slots, dtype=jnp.int32
    )
    return jnp.argsort(order_keys)[:MOVE_MAX]


def body(latents, timestep, target, qkv_weight, mod_weight, out_weight):
    slots = latents.shape[1]
    home_section = lax.axis_index("section")
    prev_section = jnp.maximum(home_section - 1, 0)
    own_steps = lax.dynamic_slice_in_dim(timestep, home_section * slots, slots)
    own_target = lax.dynamic_slice_in_dim(target, home_section * slots, slots)
    prev_steps = lax.dynamic_slice_in_dim(timestep, prev_section * slots, slots)
    prev_target = lax.dynamic_slice_in_dim(target, prev_section * slots, slots)
    own_move = own_target != home_section
    prev_move = prev_target == home_section
    qkv_local = qkv_weight[0]
    mod_table = mod_weight[0]
    out_local = out_weight[0]
    own_order = movers_first(own_move, slots)
    prev_order = movers_first(prev_move, slots)
    outgoing = jnp.take(latents, own_order, axis=1)
    incoming = from_behind(outgoing, "section", 1)
    batch = jnp.concatenate([latents, incoming], axis=1)
    steps = jnp.concatenate([own_steps, jnp.take(prev_steps, prev_order, axis=0)], axis=0)
    result = expert_block(batch, steps, qkv_local, mod_table, out_local)
    coming_back = from_behind(result[:, slots:], "section", -1)
    placing = own_order[None, :] == jnp.arange(slots, dtype=jnp.int32)[:, None]
    returned = jnp.einsum(
        "lm,sme->sle", placing.astype(jnp.bfloat16), coming_back, preferred_element_type=jnp.float32
    ).astype(jnp.bfloat16)
    return jnp.where(own_move[None, :, None], returned, result[:, :slots])


MESH = pl.DeviceIdType.MESH
F32 = jnp.float32
BF16 = jnp.bfloat16
CHUNKS = 4


def block_kernel(
    sections, target, latents, mods, w_qkv_hbm, w_out_hbm,
    updated,
    gathered, w_out, w_qkv, qkv, mix_send, mix_recv, mods_in, back, back_in,
    load_sem, send_sem, recv_sem, mix_send_sem, mix_recv_sem, hand_sem, share_sem, mods_sem,
    back_sem,
):
    tok = latents.shape[0]
    width = w_qkv.shape[1]
    slots = latents.shape[1] // width
    local = w_out.shape[2]
    heads = local // HEAD_DIM
    peers = gathered.shape[1]
    cols = width // CHUNKS
    section = lax.axis_index("section")
    me = lax.axis_index("tp")
    core = me % 2
    x = (me // 2) % 2
    y = me // 4
    to_x = 2 - 4 * x
    to_y = 4 - 8 * y
    to_c = 1 - 2 * core
    dev_x, dev_y, dev_c = me + to_x, me + to_y, me + to_c
    diag = me + to_x + to_y
    has_prev = section > 0
    has_next = section < sections - 1

    load_qkv = pltpu.make_async_copy(w_qkv_hbm, w_qkv, load_sem.at[CHUNKS])
    load_out = [
        pltpu.make_async_copy(
            w_out_hbm.at[:, j * cols : (j + 1) * cols], w_out.at[j, me], load_sem.at[j]
        )
        for j in range(CHUNKS)
    ]
    for copy in load_out:
        copy.start()
    load_qkv.start()

    barrier = pltpu.get_barrier_semaphore()
    for step in range(1, peers):
        pl.semaphore_signal(
            barrier, inc=1, device_id=(section, (me + step) % peers), device_id_type=MESH
        )

    @pl.when(has_prev)
    def _():
        pl.semaphore_signal(barrier, inc=1, device_id=(section - 1, me), device_id_type=MESH)

    @pl.when(has_next)
    def _():
        pl.semaphore_signal(barrier, inc=1, device_id=(section + 1, me), device_id_type=MESH)

    beside = jnp.minimum(section, 1) + jnp.minimum(sections - 1 - section, 1)
    pl.semaphore_wait(barrier, peers - 1 + beside)

    def mods_copy():
        return pltpu.make_async_remote_copy(
            mods.at[2], mods_in.at[0], mods_sem.at[0], mods_sem.at[1],
            device_id=(section - 1, me), device_id_type=MESH,
        )

    def back_copy(j):
        return pltpu.make_async_remote_copy(
            back.at[j], back_in.at[j], back_sem.at[0, j], back_sem.at[1, j],
            device_id=(section - 1, me), device_id_type=MESH,
        )

    @pl.when(has_prev)
    def _():
        mods_copy().start()

    flags = [(target[section * slots + j] != section).astype(jnp.int32) for j in range(slots)]
    any_move = jnp.maximum(flags[0], flags[1])

    def mask(flag, shape):
        return jnp.broadcast_to(flag, shape) != 0

    def piece(item, owner, part):
        kind, j = item
        ref = w_out if kind == "w" else gathered
        rows = ref.shape[2]
        if part is None:
            return ref.at[j, owner]
        return ref.at[j, owner, pl.ds(part * (rows // 2), rows // 2)]

    items = [("w", 0), ("t", 0), ("t", 1)] + [("w", j) for j in range(1, CHUNKS)]
    sends = [
        (me, None, dev_x), (me, None, dev_y), (me, None, dev_c),
        (dev_x, 0, dev_y), (dev_x, None, dev_c),
        (dev_y, 1, dev_x), (dev_y, None, dev_c),
        (diag, 0, dev_c), (diag, 1, dev_c),
    ]
    comes = [
        dev_x, dev_y, dev_c, diag, dev_x + to_c, diag, dev_y + to_c, diag + to_c, diag + to_c,
    ]

    def send(n, kind):
        owner, part, target = sends[kind]
        ref = piece(items[n], owner, part)
        return pltpu.make_async_remote_copy(
            ref, ref, send_sem.at[n, kind], recv_sem.at[n, kind],
            device_id=(section, target), device_id_type=MESH,
        )

    def arrive(n, kind):
        _, part, target = sends[kind]
        ref = piece(items[n], comes[kind], part)
        pltpu.make_async_remote_copy(
            ref, ref, send_sem.at[n, kind], recv_sem.at[n, kind],
            device_id=(section, target), device_id_type=MESH,
        ).wait_recv()

    handed = [(me, None), (dev_x, None), (dev_y, None), (diag, 0), (diag, 1)]

    def hand_copy(k):
        owner, part = handed[k]
        return pltpu.make_async_remote_copy(
            piece(("t", 0), owner, part), piece(("t", 2), owner, part),
            hand_sem.at[0, k], hand_sem.at[1, k],
            device_id=(section + 1, me), device_id_type=MESH,
        )

    def hand(k):
        @pl.when(has_next)
        def _():
            hand_copy(k).start()

    def share_copy(k, shift):
        owner, part = handed[k]
        ref = piece(("t", 2), owner + shift, part)
        return pltpu.make_async_remote_copy(
            ref, ref, share_sem.at[0, k], share_sem.at[1, k],
            device_id=(section, dev_c), device_id_type=MESH,
        )

    def share(*ks):
        @pl.when(has_prev)
        def _():
            for k in ks:
                hand_copy(k).wait_recv()
                share_copy(k, 0).start()

    def shared(*ks):
        @pl.when(has_prev)
        def _():
            for k in ks:
                share_copy(k, to_c).wait_recv()

    def own(slot, rows, at):
        first = latents[rows, at]
        second = latents[rows, slice(width + at.start, width + at.stop)]
        pick = mask(flags[0], first.shape)
        return jnp.where(pick, first, second) if slot == 0 else jnp.where(pick, second, first)

    def norm(slot):
        shift = mods[slot, 0:1, :]
        scale = mods[slot, 1:2, :]
        if slot == 0:
            moved = mask(any_move, shift.shape)
            shift = jnp.where(moved, mods_in[0, 0:1, :], shift)
            scale = jnp.where(moved, mods_in[0, 1:2, :], scale)
        scale = 1.0 + scale

        def rows16(i, _):
            rows = pl.ds(pl.multiple_of(i * 16, 16), 16)
            values = own(slot, rows, slice(0, width)).astype(F32)
            centred = values - jnp.mean(values, axis=-1, keepdims=True)
            variance = jnp.mean(centred * centred, axis=-1, keepdims=True)
            gathered[slot, me, rows, :] = (
                centred * lax.rsqrt(variance + 1e-06) * scale + shift
            ).astype(BF16)
            return 0

        lax.fori_loop(0, tok // 16, rows16, 0)

    def begin(n):
        kind, j = items[n]
        if kind == "w":
            load_out[j].wait()
        for kind_sent in (0, 1, 2):
            send(n, kind_sent).start()

    def forward(n):
        arrive(n, 0)
        send(n, 3).start()
        send(n, 4).start()
        if n == t0:
            hand(1)
        arrive(n, 1)
        send(n, 5).start()
        send(n, 6).start()
        if n == t0:
            hand(2)

    def last_forward(n):
        arrive(n, 3)
        send(n, 7).start()
        if n == t0:
            hand(3)
        arrive(n, 5)
        send(n, 8).start()
        if n == t0:
            hand(4)

    def mix_copy(slot, step, owner, target):
        return pltpu.make_async_remote_copy(
            mix_send.at[slot, target],
            mix_recv.at[slot, :, pl.ds(pl.multiple_of(owner * local, local), local)],
            mix_send_sem.at[slot, step], mix_recv_sem.at[slot, step],
            device_id=(section, target), device_id_type=MESH,
        )

    def project(slot, first, end):
        def step(k, _):
            chip = (y + k // 2) % 2 * 2 + (x + k % 2) % 2
            hidden = gathered[slot, pl.ds(2 * chip, 2)].reshape(2 * tok, width)
            rows = pl.ds(pl.multiple_of(chip * 2 * tok, 2 * tok), 2 * tok)
            for part in range(3):
                qkv[slot, rows, part * local : (part + 1) * local] = jnp.dot(
                    hidden, w_qkv[part], preferred_element_type=F32
                ).astype(BF16)
            return 0

        lax.fori_loop(first, end, step, 0)

    def queries(slot, first, end):
        def step(i, _):
            rows = pl.ds(pl.multiple_of(i * 2 * tok, 2 * tok), 2 * tok)
            for h in range(heads):
                a = h * HEAD_DIM
                query = qkv[slot, rows, a : a + HEAD_DIM]
                keys = qkv[slot, :, local + a : local + a + HEAD_DIM]
                vals = qkv[slot, :, 2 * local + a : 2 * local + a + HEAD_DIM]
                scores = lax.dot_general(
                    query, keys, (((1,), (1,)), ((), ())), preferred_element_type=F32
                )
                top = jnp.max(scores, axis=-1, keepdims=True)
                probs = jnp.exp((scores - top) * HEAD_DIM ** (-0.5))
                total = jnp.sum(probs, axis=-1, keepdims=True)
                mixed = jnp.dot(probs.astype(BF16), vals, preferred_element_type=F32) / total
                mix_send[slot, pl.ds(2 * i, 2), :, a : a + HEAD_DIM] = mixed.astype(
                    BF16
                ).reshape(2, tok, HEAD_DIM)
            return 0

        lax.fori_loop(first, end, step, 0)

    def exchange(slot):
        mix_recv[slot, :, pl.ds(pl.multiple_of(me * local, local), local)] = mix_send[slot, me]
        for step in range(1, peers):
            mix_copy(slot, step, me, (me + step) % peers).start()

    def mix_arrive(slot):
        for step in range(1, peers):
            mix_copy(slot, step, (me + peers - step) % peers, (me + step) % peers).wait_recv()

    def project_out(j):
        table = w_out[j].reshape(peers * local, cols)
        at = slice(j * cols, (j + 1) * cols)
        proj = jnp.dot(mix_recv[2], table, preferred_element_type=F32)
        back[j] = (mods[2, 2:3, at] * proj).astype(BF16)

        @pl.when(has_prev)
        def _():
            back_copy(j).start()

        values = []
        for slot in range(slots):
            proj = jnp.dot(mix_recv[slot], table, preferred_element_type=F32)
            raw = own(slot, slice(None), at).astype(F32)
            values.append((raw + mods[slot, 2:3, at] * proj).astype(BF16))
        pick = mask(flags[0], values[0].shape)
        updated[:, at] = jnp.where(pick, values[0], values[1])
        updated[:, slice(width + at.start, width + at.stop)] = jnp.where(
            pick, values[1], values[0]
        )

    half = peers // 4
    w0, t0, t1, w1, w2, w3 = range(len(items))
    begin(w0)

    @pl.when(has_next)
    def _():
        mods_copy().wait_recv()

    norm(0)
    begin(t0)
    hand(0)
    norm(1)
    begin(t1)
    forward(w0)
    load_qkv.wait()
    forward(t0)
    share(0)
    for kind in (2, 4, 6):
        arrive(t0, kind)
    project(0, 0, 3)
    last_forward(w0)
    forward(t1)
    begin(w1)
    for kind in (2, 4, 6):
        arrive(t1, kind)
    project(1, 0, 3)
    last_forward(t0)
    for kind in (7, 8):
        arrive(t0, kind)
    project(0, 3, 4)
    share(1)
    queries(0, 0, half)
    begin(w2)
    last_forward(t1)
    queries(0, half, 2 * half)
    exchange(0)
    for kind in (7, 8):
        arrive(t1, kind)
    share(2)
    project(1, 3, 4)
    forward(w1)
    queries(1, 0, half)
    begin(w3)
    forward(w2)
    share(3, 4)
    queries(1, half, 2 * half)
    exchange(1)
    last_forward(w1)
    shared(0, 1, 2, 3, 4)
    project(2, 0, 4)
    forward(w3)
    queries(2, 0, half)
    last_forward(w2)
    queries(2, half, 2 * half)
    exchange(2)
    last_forward(w3)
    for kind in (2, 4, 6, 7, 8):
        arrive(w0, kind)
    for slot in range(3):
        mix_arrive(slot)
    project_out(0)
    for n, j in ((w1, 1), (w2, 2), (w3, 3)):
        for kind in (2, 4, 6, 7, 8):
            arrive(n, kind)
        project_out(j)

    for j in range(CHUNKS):
        @pl.when(has_next)
        def _():
            back_copy(j).wait_recv()

        for slot in range(slots):
            at = slice(slot * width + j * cols, slot * width + (j + 1) * cols)
            for i in range(tok // 16):
                rows = slice(i * 16, (i + 1) * 16)
                returned = latents[rows, at].astype(F32) + back_in[j, rows, :].astype(F32)
                updated[rows, at] = jnp.where(
                    mask(flags[slot], (16, cols)), returned.astype(BF16), updated[rows, at]
                )

        @pl.when(has_prev)
        def _():
            back_copy(j).wait_send()

    @pl.when(has_next)
    def _():
        for k in range(len(handed)):
            hand_copy(k).wait_send()

    @pl.when(has_prev)
    def _():
        mods_copy().wait_send()
        for k in range(len(handed)):
            share_copy(k, 0).wait_send()

    for n in range(len(items)):
        for kind in range(len(sends)):
            send(n, kind).wait_send()
    for slot in range(3):
        for step in range(1, peers):
            mix_copy(slot, step, me, (me + step) % peers).wait_send()


def kernel_body(sections, latents, timestep, target, qkv_weight, mod_weight, out_weight):
    tok, slots, width = latents.shape
    local = out_weight.shape[1]
    peers = width // local
    home = lax.axis_index("section")
    prev = jnp.maximum(home - 1, 0)
    own_steps = lax.dynamic_slice_in_dim(timestep, home * slots, slots)
    prev_steps = lax.dynamic_slice_in_dim(timestep, prev * slots, slots)
    prev_move = lax.dynamic_slice_in_dim(target, prev * slots, slots) == home
    came = jnp.sum(jnp.where(prev_move, prev_steps, 0), keepdims=True)
    first = lax.dynamic_slice_in_dim(target, home * slots, 1) != home
    turned = jnp.where(first, own_steps, own_steps[::-1])
    mods = modulate(jnp.concatenate([turned, came]), mod_weight[0])
    vmem = pl.BlockSpec(memory_space=pltpu.VMEM)
    hbm = pl.BlockSpec(memory_space=pl.ANY)
    cols = width // CHUNKS
    n_items = slots + CHUNKS
    dma = pltpu.SemaphoreType.DMA
    updated = pl.pallas_call(
        functools.partial(block_kernel, sections),
        out_shape=jax.ShapeDtypeStruct((tok, slots * width), BF16),
        in_specs=[pl.BlockSpec(memory_space=pltpu.SMEM), vmem, vmem, hbm, hbm],
        out_specs=vmem,
        scratch_shapes=[
            pltpu.VMEM((slots + 1, peers, tok, width), BF16),
            pltpu.VMEM((CHUNKS, peers, local, cols), BF16),
            pltpu.VMEM((3, width, local), BF16),
            pltpu.VMEM((slots + 1, peers * tok, 3 * local), BF16),
            pltpu.VMEM((slots + 1, peers, tok, local), BF16),
            pltpu.VMEM((slots + 1, tok, width), BF16),
            pltpu.VMEM((1, 3, width), F32),
            pltpu.VMEM((CHUNKS, tok, cols), BF16),
            pltpu.VMEM((CHUNKS, tok, cols), BF16),
            dma((CHUNKS + 1,)),
            dma((n_items, 9)),
            dma((n_items, 9)),
            dma((slots + 1, peers)),
            dma((slots + 1, peers)),
            dma((2, 5)),
            dma((2, 5)),
            dma((2,)),
            dma((2, CHUNKS)),
        ],
        compiler_params=pltpu.CompilerParams(
            collective_id=0, has_side_effects=True, vmem_limit_bytes=60 * 1024 * 1024
        ),
    )(
        target,
        latents.reshape(tok, slots * width),
        mods,
        jnp.transpose(qkv_weight[0], (1, 0, 2)),
        out_weight[0],
    )
    return updated.reshape(tok, slots, width)


def solution(mesh):
    sections = mesh.shape["section"]
    plan = functools.partial(kernel_body, sections) if mesh.shape["tp"] == 8 else body

    return jax.shard_map(
        plan,
        mesh=mesh,
        in_specs=(
            P("tp", "section", None),
            P(),
            P(),
            P("section", None, None, "tp"),
            P("section", None, None, None),
            P("section", "tp", None),
        ),
        out_specs=P("tp", "section", None),
        check_vma=False,
    )
```

```python
import functools
import math

import jax
import jax.numpy as jnp
from jax import lax
from jax.experimental import pallas as pl
from jax.experimental.pallas import tpu as pltpu
from jax.sharding import PartitionSpec as P

HEAD_DIM = 128
FREQ = 256
MOVE_MAX = 1


def from_behind(shard, axis, by):
    peers = lax.axis_size(axis)
    pairs = [(i, i + by) for i in range(peers) if 0 <= i + by < peers]
    return lax.ppermute(shard, axis, pairs)


def time_embed(steps):
    half_width = FREQ // 2
    frequency = jnp.exp(-math.log(10000.0) * jnp.arange(half_width, dtype=jnp.float32) / half_width)
    angles = steps.astype(jnp.float32)[:, None] * frequency[None, :]
    return jnp.concatenate([jnp.cos(angles), jnp.sin(angles)], axis=1)


def modulate(steps, mod_table):
    feature = jax.nn.silu(time_embed(steps))
    return jnp.einsum(
        "bf,fcd->bcd", feature, mod_table.astype(jnp.float32), precision=lax.Precision.HIGHEST
    )


def normalize(values, shift, scale):
    row_mean = jnp.mean(values, axis=-1, keepdims=True)
    centred = values - row_mean
    variance = jnp.mean(centred * centred, axis=-1, keepdims=True)
    return centred * lax.rsqrt(variance + 1e-06) * (1.0 + scale) + shift


def expert_block(batch, steps, qkv_local, mod_table, out_local):
    mods = modulate(steps, mod_table)
    values = batch.astype(jnp.float32)
    hidden = normalize(values, mods[None, :, 0], mods[None, :, 1]).astype(jnp.bfloat16)
    packed = jnp.einsum(
        "sbd,dce->sbce",
        lax.all_gather(hidden, "tp", axis=0, tiled=True),
        qkv_local,
        preferred_element_type=jnp.float32,
    ).astype(jnp.bfloat16)
    tok_all = packed.shape[0]
    slot_count = packed.shape[1]
    local_width = packed.shape[3]
    head_local = local_width // HEAD_DIM
    split_heads = packed.reshape(tok_all, slot_count, 3, head_local, HEAD_DIM)
    query = split_heads[:, :, 0]
    keys_now = split_heads[:, :, 1]
    vals_now = split_heads[:, :, 2]
    scores = jnp.einsum(
        "qbhe,kbhe->bhqk", query, keys_now, preferred_element_type=jnp.float32
    ) * HEAD_DIM ** (-0.5)
    soft = jax.nn.softmax(scores, axis=-1).astype(jnp.bfloat16)
    mixed = jnp.einsum("bhqk,kbhe->qbhe", soft, vals_now, preferred_element_type=jnp.float32)
    mixed = mixed.astype(jnp.bfloat16).reshape(tok_all, slot_count, local_width)
    proj = lax.psum_scatter(
        jnp.einsum("sbk,kd->sbd", mixed, out_local, preferred_element_type=jnp.float32).astype(
            jnp.bfloat16
        ),
        "tp",
        scatter_dimension=0,
        tiled=True,
    ).astype(jnp.float32)
    return (values + mods[None, :, 2] * proj).astype(jnp.bfloat16)


def movers_first(move_flags, slots):
    order_keys = jnp.where(move_flags, 0, 1).astype(jnp.int32) * slots + jnp.arange(
        slots, dtype=jnp.int32
    )
    return jnp.argsort(order_keys)[:MOVE_MAX]


def body(latents, timestep, target, qkv_weight, mod_weight, out_weight):
    slots = latents.shape[1]
    home_section = lax.axis_index("section")
    prev_section = jnp.maximum(home_section - 1, 0)
    own_steps = lax.dynamic_slice_in_dim(timestep, home_section * slots, slots)
    own_target = lax.dynamic_slice_in_dim(target, home_section * slots, slots)
    prev_steps = lax.dynamic_slice_in_dim(timestep, prev_section * slots, slots)
    prev_target = lax.dynamic_slice_in_dim(target, prev_section * slots, slots)
    own_move = own_target != home_section
    prev_move = prev_target == home_section
    qkv_local = qkv_weight[0]
    mod_table = mod_weight[0]
    out_local = out_weight[0]
    own_order = movers_first(own_move, slots)
    prev_order = movers_first(prev_move, slots)
    outgoing = jnp.take(latents, own_order, axis=1)
    incoming = from_behind(outgoing, "section", 1)
    batch = jnp.concatenate([latents, incoming], axis=1)
    steps = jnp.concatenate([own_steps, jnp.take(prev_steps, prev_order, axis=0)], axis=0)
    result = expert_block(batch, steps, qkv_local, mod_table, out_local)
    coming_back = from_behind(result[:, slots:], "section", -1)
    placing = own_order[None, :] == jnp.arange(slots, dtype=jnp.int32)[:, None]
    returned = jnp.einsum(
        "lm,sme->sle", placing.astype(jnp.bfloat16), coming_back, preferred_element_type=jnp.float32
    ).astype(jnp.bfloat16)
    return jnp.where(own_move[None, :, None], returned, result[:, :slots])


MESH = pl.DeviceIdType.MESH
F32 = jnp.float32
BF16 = jnp.bfloat16
CHUNKS = 4


def block_kernel(
    sections, target, timestep, latents_hbm, w_mod_hbm, w_qkv_hbm, w_out_hbm,
    updated_hbm,
    latents, raw, w_mod, mods, mods_out, mods_in, gathered, w_out, w_qkv, qkv, mix_send, mix_recv,
    back, back_in, hold, updated,
    load_sem, send_sem, recv_sem, mix_send_sem, mix_recv_sem, hand_sem, share_sem, mods_sem,
    back_sem, store_sem,
):
    tok, slots, width = latents.shape
    local = w_out.shape[2]
    heads = local // HEAD_DIM
    peers = gathered.shape[1]
    cols = width // CHUNKS
    section = lax.axis_index("section")
    me = lax.axis_index("tp")
    core = me % 2
    x = (me // 2) % 2
    y = me // 4
    to_x = 2 - 4 * x
    to_y = 4 - 8 * y
    to_c = 1 - 2 * core
    dev_x, dev_y, dev_c = me + to_x, me + to_y, me + to_c
    diag = me + to_x + to_y
    has_prev = section > 0
    has_next = section < sections - 1

    load_out = [
        pltpu.make_async_copy(
            w_out_hbm.at[:, j * cols : (j + 1) * cols], w_out.at[j, me], load_sem.at[j]
        )
        for j in range(CHUNKS)
    ]
    load_qkv = pltpu.make_async_copy(w_qkv_hbm, w_qkv, load_sem.at[CHUNKS])
    load_mod = pltpu.make_async_copy(w_mod_hbm, w_mod, load_sem.at[CHUNKS + 1])
    load_latents = pltpu.make_async_copy(latents_hbm, latents, load_sem.at[CHUNKS + 2])
    for copy in (load_out[0], load_mod, load_latents, *load_out[1:], load_qkv):
        copy.start()

    barrier = pltpu.get_barrier_semaphore()
    for step in range(1, peers):
        pl.semaphore_signal(
            barrier, inc=1, device_id=(section, (me + step) % peers), device_id_type=MESH
        )

    @pl.when(has_prev)
    def _():
        pl.semaphore_signal(barrier, inc=1, device_id=(section - 1, me), device_id_type=MESH)

    @pl.when(has_next)
    def _():
        pl.semaphore_signal(barrier, inc=1, device_id=(section + 1, me), device_id_type=MESH)

    beside = jnp.minimum(section, 1) + jnp.minimum(sections - 1 - section, 1)
    pl.semaphore_wait(barrier, peers - 1 + beside)

    def mods_copy():
        return pltpu.make_async_remote_copy(
            mods_out, mods_in, mods_sem.at[0], mods_sem.at[1],
            device_id=(section - 1, me), device_id_type=MESH,
        )

    def back_copy(j):
        return pltpu.make_async_remote_copy(
            back.at[j], back_in.at[j], back_sem.at[0, j], back_sem.at[1, j],
            device_id=(section - 1, me), device_id_type=MESH,
        )

    flags = [(target[section * slots + j] != section).astype(jnp.int32) for j in range(slots)]
    any_move = jnp.maximum(flags[0], flags[1])

    def mask(flag, shape):
        return jnp.broadcast_to(flag, shape) != 0

    def piece(item, owner, part):
        kind, j = item
        ref = w_out if kind == "w" else gathered
        rows = ref.shape[2]
        if part is None:
            return ref.at[j, owner]
        return ref.at[j, owner, pl.ds(part * (rows // 2), rows // 2)]

    items = [("w", 0), ("t", 0), ("t", 1)] + [("w", j) for j in range(1, CHUNKS)]
    sends = [
        (me, None, dev_x), (me, None, dev_y), (me, None, dev_c),
        (dev_x, 0, dev_y), (dev_x, None, dev_c),
        (dev_y, 1, dev_x), (dev_y, None, dev_c),
        (diag, 0, dev_c), (diag, 1, dev_c),
    ]
    comes = [
        dev_x, dev_y, dev_c, diag, dev_x + to_c, diag, dev_y + to_c, diag + to_c, diag + to_c,
    ]

    def send(n, kind):
        owner, part, target = sends[kind]
        ref = piece(items[n], owner, part)
        return pltpu.make_async_remote_copy(
            ref, ref, send_sem.at[n, kind], recv_sem.at[n, kind],
            device_id=(section, target), device_id_type=MESH,
        )

    def arrive(n, kind):
        _, part, target = sends[kind]
        ref = piece(items[n], comes[kind], part)
        pltpu.make_async_remote_copy(
            ref, ref, send_sem.at[n, kind], recv_sem.at[n, kind],
            device_id=(section, target), device_id_type=MESH,
        ).wait_recv()

    handed = [(me, None), (dev_x, None), (dev_y, None), (diag, 0), (diag, 1)]

    def hand_copy(k):
        owner, part = handed[k]
        return pltpu.make_async_remote_copy(
            piece(("t", 0), owner, part), piece(("t", 2), owner, part),
            hand_sem.at[0, k], hand_sem.at[1, k],
            device_id=(section + 1, me), device_id_type=MESH,
        )

    def hand(k):
        @pl.when(has_next)
        def _():
            hand_copy(k).start()

    def share_copy(k, shift):
        owner, part = handed[k]
        ref = piece(("t", 2), owner + shift, part)
        return pltpu.make_async_remote_copy(
            ref, ref, share_sem.at[0, k], share_sem.at[1, k],
            device_id=(section, dev_c), device_id_type=MESH,
        )

    def share(*ks):
        @pl.when(has_prev)
        def _():
            for k in ks:
                hand_copy(k).wait_recv()
                share_copy(k, 0).start()

    def shared(*ks):
        @pl.when(has_prev)
        def _():
            for k in ks:
                share_copy(k, to_c).wait_recv()

    def modulation():
        prev = jnp.maximum(section - 1, 0)
        came = sum(
            jnp.where(target[prev * slots + j] == section, timestep[prev * slots + j], 0)
            for j in range(slots)
        )
        step0, step1 = timestep[section * slots], timestep[section * slots + 1]
        step_a = jnp.where(flags[0] != 0, step0, step1)
        step_b = jnp.where(flags[0] != 0, step1, step0)
        half_width = FREQ // 2
        row = lax.broadcasted_iota(jnp.int32, (8, half_width), 0)
        steps = jnp.where(row == 0, step_a, jnp.where(row == 1, step_b, came)).astype(F32)
        lane = lax.broadcasted_iota(jnp.int32, (8, half_width), 1).astype(F32)
        angles = steps * jnp.exp(-math.log(10000.0) * lane / half_width)
        embed = jnp.concatenate([jnp.cos(angles), jnp.sin(angles)], axis=1)
        rest = embed / (1.0 + jnp.exp(-embed))
        terms = []
        for _ in range(3):
            terms.append(rest.astype(BF16).astype(F32))
            rest = rest - terms[-1]
        terms = jnp.concatenate(terms, axis=0).astype(BF16)
        load_mod.wait()
        for part in range(3):
            sums = jnp.dot(terms, w_mod[part], preferred_element_type=F32)
            mods[part] = sums[0:8] + sums[8:16] + sums[16:24]
        quarter = width // 4
        for part in range(2):
            for q in range(4):
                mods_out[part * 4 + q : part * 4 + q + 1, :] = mods[
                    part, 2:3, q * quarter : (q + 1) * quarter
                ]

        @pl.when(has_prev)
        def _():
            mods_copy().start()

    def unpack():
        for i in range(tok // 16):
            rows = slice(i * 16, (i + 1) * 16)
            both = pltpu.einshape("asc->sac", latents[rows])
            pick = mask(flags[0], (16, width))
            raw[0, rows, :] = jnp.where(pick, both[0], both[1])
            raw[1, rows, :] = jnp.where(pick, both[1], both[0])

    def norm(slot):
        shift = mods[0, slot : slot + 1, :]
        scale = mods[1, slot : slot + 1, :]
        if slot == 0:
            moved = mask(any_move, shift.shape)
            came = [
                jnp.concatenate([mods_in[4 * part + q : 4 * part + q + 1, :] for q in range(4)], axis=1)
                for part in range(2)
            ]
            shift = jnp.where(moved, came[0], shift)
            scale = jnp.where(moved, came[1], scale)
        scale = 1.0 + scale

        def rows16(i, _):
            rows = pl.ds(pl.multiple_of(i * 16, 16), 16)
            values = raw[slot, rows, :].astype(F32)
            centred = values - jnp.mean(values, axis=-1, keepdims=True)
            variance = jnp.mean(centred * centred, axis=-1, keepdims=True)
            gathered[slot, me, rows, :] = (
                centred * lax.rsqrt(variance + 1e-06) * scale + shift
            ).astype(BF16)
            return 0

        lax.fori_loop(0, tok // 16, rows16, 0)

    def begin(n):
        kind, j = items[n]
        if kind == "w":
            load_out[j].wait()
        for kind_sent in (0, 1, 2):
            send(n, kind_sent).start()

    def forward(n):
        arrive(n, 0)
        send(n, 3).start()
        send(n, 4).start()
        if n == t0:
            hand(1)
        arrive(n, 1)
        send(n, 5).start()
        send(n, 6).start()
        if n == t0:
            hand(2)

    def last_forward(n):
        arrive(n, 3)
        send(n, 7).start()
        if n == t0:
            hand(3)
        arrive(n, 5)
        send(n, 8).start()
        if n == t0:
            hand(4)

    def mix_copy(slot, step, owner, target):
        return pltpu.make_async_remote_copy(
            mix_send.at[slot, target],
            mix_recv.at[slot, :, pl.ds(pl.multiple_of(owner * local, local), local)],
            mix_send_sem.at[slot, step], mix_recv_sem.at[slot, step],
            device_id=(section, target), device_id_type=MESH,
        )

    def project(slot, first, end):
        def step(k, _):
            chip = (y + k // 2) % 2 * 2 + (x + k % 2) % 2
            hidden = gathered[slot, pl.ds(2 * chip, 2)].reshape(2 * tok, width)
            rows = pl.ds(pl.multiple_of(chip * 2 * tok, 2 * tok), 2 * tok)
            for part in range(3):
                qkv[slot, rows, part * local : (part + 1) * local] = jnp.dot(
                    hidden, w_qkv[part], preferred_element_type=F32
                ).astype(BF16)
            return 0

        lax.fori_loop(first, end, step, 0)

    def queries(slot, first, end):
        def step(i, _):
            rows = pl.ds(pl.multiple_of(i * 2 * tok, 2 * tok), 2 * tok)
            for h in range(heads):
                a = h * HEAD_DIM
                query = qkv[slot, rows, a : a + HEAD_DIM]
                keys = qkv[slot, :, local + a : local + a + HEAD_DIM]
                vals = qkv[slot, :, 2 * local + a : 2 * local + a + HEAD_DIM]
                scores = lax.dot_general(
                    query, keys, (((1,), (1,)), ((), ())), preferred_element_type=F32
                )
                top = jnp.max(scores, axis=-1, keepdims=True)
                probs = jnp.exp((scores - top) * HEAD_DIM ** (-0.5))
                total = jnp.sum(probs, axis=-1, keepdims=True)
                mixed = jnp.dot(probs.astype(BF16), vals, preferred_element_type=F32) / total
                mix_send[slot, pl.ds(2 * i, 2), :, a : a + HEAD_DIM] = mixed.astype(
                    BF16
                ).reshape(2, tok, HEAD_DIM)
            return 0

        lax.fori_loop(first, end, step, 0)

    def exchange(slot):
        mix_recv[slot, :, pl.ds(pl.multiple_of(me * local, local), local)] = mix_send[slot, me]
        for step in range(1, peers):
            mix_copy(slot, step, me, (me + step) % peers).start()

    def mix_arrive(slot):
        for step in range(1, peers):
            mix_copy(slot, step, (me + peers - step) % peers, (me + step) % peers).wait_recv()

    def project_out(slot, j):
        table = w_out[j].reshape(peers * local, cols)
        at = slice(j * cols, (j + 1) * cols)
        change = mods[2, slot : slot + 1, at] * jnp.dot(
            mix_recv[slot], table, preferred_element_type=F32
        )
        if slot == 2:
            back[j] = change.astype(BF16)

            @pl.when(has_prev)
            def _():
                back_copy(j).start()

            return
        hold[slot, j] = (raw[slot, :, at].astype(F32) + change).astype(BF16)

    def store_copy(j):
        at = slice(j * cols, (j + 1) * cols)
        return pltpu.make_async_copy(
            updated.at[:, :, at], updated_hbm.at[:, :, at], store_sem.at[j]
        )

    def write(j):
        @pl.when(has_next)
        def _():
            back_copy(j).wait_recv()

        at = slice(j * cols, (j + 1) * cols)
        pick = mask(flags[0], (16, cols))
        moved = mask(any_move, (16, cols))
        for i in range(tok // 16):
            rows = slice(i * 16, (i + 1) * 16)
            returned = raw[0, rows, at].astype(F32) + back_in[j, rows, :].astype(F32)
            first = jnp.where(moved, returned.astype(BF16), hold[0, j, rows, :])
            second = hold[1, j, rows, :]
            updated[rows, 0, at] = jnp.where(pick, first, second)
            updated[rows, 1, at] = jnp.where(pick, second, first)
        store_copy(j).start()

    half = peers // 4
    w0, t0, t1, w1, w2, w3 = range(len(items))
    begin(w0)
    modulation()
    load_latents.wait()
    unpack()

    @pl.when(has_next)
    def _():
        mods_copy().wait_recv()

    norm(0)
    begin(t0)
    hand(0)
    begin(w1)
    norm(1)
    forward(w0)
    load_qkv.wait()
    arrive(t0, 2)
    project(0, 0, 1)
    forward(t0)
    begin(t1)
    for kind in (4, 6):
        arrive(t0, kind)
    project(0, 1, 3)
    share(0)
    last_forward(w0)
    forward(w1)
    last_forward(t0)
    for kind in (7, 8):
        arrive(t0, kind)
    project(0, 3, 4)
    begin(w2)
    queries(0, 0, half)
    last_forward(w1)
    queries(0, half, 2 * half)
    exchange(0)
    share(1)
    shared(0, 1)
    project(2, 0, 2)
    forward(t1)
    begin(w3)
    for kind in (2, 4, 6):
        arrive(t1, kind)
    project(1, 0, 3)
    share(2)
    forward(w2)
    last_forward(t1)
    share(3, 4)
    shared(2, 3, 4)
    project(2, 2, 4)
    queries(2, 0, half)
    last_forward(w2)
    forward(w3)
    queries(2, half, 2 * half)
    exchange(2)
    for kind in (7, 8):
        arrive(t1, kind)
    project(1, 3, 4)
    last_forward(w3)
    queries(1, 0, half)
    mix_arrive(2)
    for n, j in ((w0, 0), (w1, 1)):
        for kind in (2, 4, 6, 7, 8):
            arrive(n, kind)
        project_out(2, j)
    queries(1, half, 2 * half)
    exchange(1)
    for n, j in ((w2, 2), (w3, 3)):
        for kind in (2, 4, 6, 7, 8):
            arrive(n, kind)
        project_out(2, j)
    mix_arrive(0)
    for j in range(CHUNKS):
        project_out(0, j)
    mix_arrive(1)
    for j in range(CHUNKS):
        project_out(1, j)
        write(j)
    for j in range(CHUNKS):
        store_copy(j).wait()

        @pl.when(has_prev)
        def _():
            back_copy(j).wait_send()

    @pl.when(has_next)
    def _():
        for k in range(len(handed)):
            hand_copy(k).wait_send()

    @pl.when(has_prev)
    def _():
        mods_copy().wait_send()
        for k in range(len(handed)):
            share_copy(k, 0).wait_send()

    for n in range(len(items)):
        for kind in range(len(sends)):
            send(n, kind).wait_send()
    for slot in range(3):
        for step in range(1, peers):
            mix_copy(slot, step, me, (me + step) % peers).wait_send()


def kernel_body(sections, latents, timestep, target, qkv_weight, mod_weight, out_weight):
    tok, slots, width = latents.shape
    local = out_weight.shape[1]
    peers = width // local
    smem = pl.BlockSpec(memory_space=pltpu.SMEM)
    hbm = pl.BlockSpec(memory_space=pl.ANY)
    cols = width // CHUNKS
    n_items = slots + CHUNKS
    dma = pltpu.SemaphoreType.DMA
    updated = pl.pallas_call(
        functools.partial(block_kernel, sections),
        out_shape=jax.ShapeDtypeStruct((tok, slots, width), BF16),
        in_specs=[smem, smem, hbm, hbm, hbm, hbm],
        out_specs=hbm,
        scratch_shapes=[
            pltpu.VMEM((tok, slots, width), BF16),
            pltpu.VMEM((slots, tok, width), BF16),
            pltpu.VMEM((3, FREQ, width), BF16),
            pltpu.VMEM((3, 8, width), F32),
            pltpu.VMEM((8, width // 4), F32),
            pltpu.VMEM((8, width // 4), F32),
            pltpu.VMEM((slots + 1, peers, tok, width), BF16),
            pltpu.VMEM((CHUNKS, peers, local, cols), BF16),
            pltpu.VMEM((3, width, local), BF16),
            pltpu.VMEM((slots + 1, peers * tok, 3 * local), BF16),
            pltpu.VMEM((slots + 1, peers, tok, local), BF16),
            pltpu.VMEM((slots + 1, tok, width), BF16),
            pltpu.VMEM((CHUNKS, tok, cols), BF16),
            pltpu.VMEM((CHUNKS, tok, cols), BF16),
            pltpu.VMEM((slots, CHUNKS, tok, cols), BF16),
            pltpu.VMEM((tok, slots, width), BF16),
            dma((CHUNKS + 3,)),
            dma((n_items, 9)),
            dma((n_items, 9)),
            dma((slots + 1, peers)),
            dma((slots + 1, peers)),
            dma((2, 5)),
            dma((2, 5)),
            dma((2,)),
            dma((2, CHUNKS)),
            dma((CHUNKS,)),
        ],
        compiler_params=pltpu.CompilerParams(
            collective_id=0, has_side_effects=True, vmem_limit_bytes=60 * 1024 * 1024
        ),
    )(
        target,
        timestep,
        latents,
        jnp.transpose(mod_weight[0], (1, 0, 2)),
        jnp.transpose(qkv_weight[0], (1, 0, 2)),
        out_weight[0],
    )
    return updated


def solution(mesh):
    sections = mesh.shape["section"]
    plan = functools.partial(kernel_body, sections) if mesh.shape["tp"] == 8 else body

    return jax.shard_map(
        plan,
        mesh=mesh,
        in_specs=(
            P("tp", "section", None),
            P(),
            P(),
            P("section", None, None, "tp"),
            P("section", None, None, None),
            P("section", "tp", None),
        ),
        out_specs=P("tp", "section", None),
        check_vma=False,
    )
```

```python
import functools
import math

import jax
import jax.numpy as jnp
from jax import lax
from jax.experimental import pallas as pl
from jax.experimental.pallas import tpu as pltpu
from jax.sharding import PartitionSpec as P

HEAD_DIM = 128
FREQ = 256
MOVE_MAX = 1


def from_behind(shard, axis, by):
    peers = lax.axis_size(axis)
    pairs = [(i, i + by) for i in range(peers) if 0 <= i + by < peers]
    return lax.ppermute(shard, axis, pairs)


def time_embed(steps):
    half_width = FREQ // 2
    frequency = jnp.exp(-math.log(10000.0) * jnp.arange(half_width, dtype=jnp.float32) / half_width)
    angles = steps.astype(jnp.float32)[:, None] * frequency[None, :]
    return jnp.concatenate([jnp.cos(angles), jnp.sin(angles)], axis=1)


def modulate(steps, mod_table):
    feature = jax.nn.silu(time_embed(steps))
    return jnp.einsum(
        "bf,fcd->bcd", feature, mod_table.astype(jnp.float32), precision=lax.Precision.HIGHEST
    )


def normalize(values, shift, scale):
    row_mean = jnp.mean(values, axis=-1, keepdims=True)
    centred = values - row_mean
    variance = jnp.mean(centred * centred, axis=-1, keepdims=True)
    return centred * lax.rsqrt(variance + 1e-06) * (1.0 + scale) + shift


def expert_block(batch, steps, qkv_local, mod_table, out_local):
    mods = modulate(steps, mod_table)
    values = batch.astype(jnp.float32)
    hidden = normalize(values, mods[None, :, 0], mods[None, :, 1]).astype(jnp.bfloat16)
    packed = jnp.einsum(
        "sbd,dce->sbce",
        lax.all_gather(hidden, "tp", axis=0, tiled=True),
        qkv_local,
        preferred_element_type=jnp.float32,
    ).astype(jnp.bfloat16)
    tok_all = packed.shape[0]
    slot_count = packed.shape[1]
    local_width = packed.shape[3]
    head_local = local_width // HEAD_DIM
    split_heads = packed.reshape(tok_all, slot_count, 3, head_local, HEAD_DIM)
    query = split_heads[:, :, 0]
    keys_now = split_heads[:, :, 1]
    vals_now = split_heads[:, :, 2]
    scores = jnp.einsum(
        "qbhe,kbhe->bhqk", query, keys_now, preferred_element_type=jnp.float32
    ) * HEAD_DIM ** (-0.5)
    soft = jax.nn.softmax(scores, axis=-1).astype(jnp.bfloat16)
    mixed = jnp.einsum("bhqk,kbhe->qbhe", soft, vals_now, preferred_element_type=jnp.float32)
    mixed = mixed.astype(jnp.bfloat16).reshape(tok_all, slot_count, local_width)
    proj = lax.psum_scatter(
        jnp.einsum("sbk,kd->sbd", mixed, out_local, preferred_element_type=jnp.float32).astype(
            jnp.bfloat16
        ),
        "tp",
        scatter_dimension=0,
        tiled=True,
    ).astype(jnp.float32)
    return (values + mods[None, :, 2] * proj).astype(jnp.bfloat16)


def movers_first(move_flags, slots):
    order_keys = jnp.where(move_flags, 0, 1).astype(jnp.int32) * slots + jnp.arange(
        slots, dtype=jnp.int32
    )
    return jnp.argsort(order_keys)[:MOVE_MAX]


def body(latents, timestep, target, qkv_weight, mod_weight, out_weight):
    slots = latents.shape[1]
    home_section = lax.axis_index("section")
    prev_section = jnp.maximum(home_section - 1, 0)
    own_steps = lax.dynamic_slice_in_dim(timestep, home_section * slots, slots)
    own_target = lax.dynamic_slice_in_dim(target, home_section * slots, slots)
    prev_steps = lax.dynamic_slice_in_dim(timestep, prev_section * slots, slots)
    prev_target = lax.dynamic_slice_in_dim(target, prev_section * slots, slots)
    own_move = own_target != home_section
    prev_move = prev_target == home_section
    qkv_local = qkv_weight[0]
    mod_table = mod_weight[0]
    out_local = out_weight[0]
    own_order = movers_first(own_move, slots)
    prev_order = movers_first(prev_move, slots)
    outgoing = jnp.take(latents, own_order, axis=1)
    incoming = from_behind(outgoing, "section", 1)
    batch = jnp.concatenate([latents, incoming], axis=1)
    steps = jnp.concatenate([own_steps, jnp.take(prev_steps, prev_order, axis=0)], axis=0)
    result = expert_block(batch, steps, qkv_local, mod_table, out_local)
    coming_back = from_behind(result[:, slots:], "section", -1)
    placing = own_order[None, :] == jnp.arange(slots, dtype=jnp.int32)[:, None]
    returned = jnp.einsum(
        "lm,sme->sle", placing.astype(jnp.bfloat16), coming_back, preferred_element_type=jnp.float32
    ).astype(jnp.bfloat16)
    return jnp.where(own_move[None, :, None], returned, result[:, :slots])


MESH = pl.DeviceIdType.MESH
F32 = jnp.float32
BF16 = jnp.bfloat16
CHUNKS = 4


def block_kernel(
    sections, target, timestep, latents_hbm, w_mod_hbm, w_qkv_hbm, w_out_hbm,
    updated_hbm,
    latents, raw, w_mod, mods, mods_out, mods_in, gathered, w_out, w_qkv, qkv, mix_send, mix_recv,
    part, part_send, part_recv, back, back_in, hold, updated,
    load_sem, send_sem, recv_sem, table_sem, mix_sem, part_sem, hand_sem, share_sem, mods_sem,
    back_sem, store_sem,
):
    tok, slots, width = latents.shape
    local = w_out.shape[2]
    heads = local // HEAD_DIM
    peers = gathered.shape[1]
    cols = width // CHUNKS
    section = lax.axis_index("section")
    me = lax.axis_index("tp")
    core = me % 2
    x = (me // 2) % 2
    y = me // 4
    to_x = 2 - 4 * x
    to_y = 4 - 8 * y
    to_c = 1 - 2 * core
    dev_x, dev_y, dev_c = me + to_x, me + to_y, me + to_c
    diag = me + to_x + to_y
    row = me % 4
    has_prev = section > 0
    has_next = section < sections - 1

    load_out = [
        pltpu.make_async_copy(
            w_out_hbm.at[:, j * cols : (j + 1) * cols], w_out.at[j, row], load_sem.at[j]
        )
        for j in range(CHUNKS)
    ]
    load_qkv = pltpu.make_async_copy(w_qkv_hbm, w_qkv, load_sem.at[CHUNKS])
    load_mod = pltpu.make_async_copy(w_mod_hbm, w_mod, load_sem.at[CHUNKS + 1])
    load_latents = pltpu.make_async_copy(latents_hbm, latents, load_sem.at[CHUNKS + 2])
    for copy in (load_out[0], load_latents, load_mod, *load_out[1:], load_qkv):
        copy.start()

    barrier = pltpu.get_barrier_semaphore()
    for step in range(1, peers):
        pl.semaphore_signal(
            barrier, inc=1, device_id=(section, (me + step) % peers), device_id_type=MESH
        )

    @pl.when(has_prev)
    def _():
        pl.semaphore_signal(barrier, inc=1, device_id=(section - 1, me), device_id_type=MESH)

    @pl.when(has_next)
    def _():
        pl.semaphore_signal(barrier, inc=1, device_id=(section + 1, me), device_id_type=MESH)

    beside = jnp.minimum(section, 1) + jnp.minimum(sections - 1 - section, 1)
    pl.semaphore_wait(barrier, peers - 1 + beside)

    def mods_copy():
        return pltpu.make_async_remote_copy(
            mods_out, mods_in, mods_sem.at[0], mods_sem.at[1],
            device_id=(section - 1, me), device_id_type=MESH,
        )

    def back_copy(j):
        return pltpu.make_async_remote_copy(
            back.at[j], back_in.at[j], back_sem.at[0, j], back_sem.at[1, j],
            device_id=(section - 1, me), device_id_type=MESH,
        )

    flags = [(target[section * slots + j] != section).astype(jnp.int32) for j in range(slots)]
    any_move = jnp.maximum(flags[0], flags[1])

    def mask(flag, shape):
        return jnp.broadcast_to(flag, shape) != 0

    def piece(slot, owner, part):
        rows = gathered.shape[2]
        if part is None:
            return gathered.at[slot, owner]
        return gathered.at[slot, owner, pl.ds(part * (rows // 2), rows // 2)]

    comes = [
        dev_x, dev_y, dev_c, diag, dev_x + to_c, diag, dev_y + to_c, diag + to_c, diag + to_c,
        dev_y,
    ]

    def route(n, kind):
        return [
            (me, None, dev_x), (me, 0, dev_y), (me, None, dev_c),
            (dev_x, 0, dev_y), (dev_x, None, dev_c),
            (dev_x, 1, dev_y), (dev_y, None, dev_c),
            (diag, 0, dev_c), (diag, 1, dev_c), (me, 1, dev_y),
        ][kind]

    def send(n, kind):
        owner, part, target = route(n, kind)
        ref = piece(n, owner, part)
        return pltpu.make_async_remote_copy(
            ref, ref, send_sem.at[n, kind], recv_sem.at[n, kind],
            device_id=(section, target), device_id_type=MESH,
        )

    def arrive(n, kind):
        _, part, target = route(n, kind)
        ref = piece(n, comes[kind], part)
        pltpu.make_async_remote_copy(
            ref, ref, send_sem.at[n, kind], recv_sem.at[n, kind],
            device_id=(section, target), device_id_type=MESH,
        ).wait_recv()

    def table_copy(j, kind, shift):
        owner, target = [(me, dev_x), (me, dev_c), (dev_x, dev_c)][kind]
        ref = w_out.at[j, (owner + shift) % 4]
        return pltpu.make_async_remote_copy(
            ref, ref, table_sem.at[0, j, kind], table_sem.at[1, j, kind],
            device_id=(section, target), device_id_type=MESH,
        )

    def table_begin(*js):
        for j in js:
            load_out[j].wait()
            table_copy(j, 0, 0).start()
            table_copy(j, 1, 0).start()

    def table_forward(*js):
        for j in js:
            table_copy(j, 0, to_x).wait_recv()
            table_copy(j, 2, 0).start()

    def table_arrive(*js):
        for j in js:
            table_copy(j, 1, to_c).wait_recv()
            table_copy(j, 2, to_c).wait_recv()

    handed = [(me, None), (dev_x, None), (dev_y, None), (diag, 0), (diag, 1)]

    def hand_copy(k):
        owner, part = handed[k]
        return pltpu.make_async_remote_copy(
            piece(0, owner, part), piece(2, owner, part),
            hand_sem.at[0, k], hand_sem.at[1, k],
            device_id=(section + 1, me), device_id_type=MESH,
        )

    def hand(k):
        @pl.when(has_next)
        def _():
            hand_copy(k).start()

    def share_copy(k, shift):
        owner, part = handed[k]
        ref = piece(2, owner + shift, part)
        return pltpu.make_async_remote_copy(
            ref, ref, share_sem.at[0, k], share_sem.at[1, k],
            device_id=(section, dev_c), device_id_type=MESH,
        )

    def share(*ks):
        @pl.when(has_prev)
        def _():
            for k in ks:
                hand_copy(k).wait_recv()
                share_copy(k, 0).start()

    def shared(*ks):
        @pl.when(has_prev)
        def _():
            for k in ks:
                share_copy(k, to_c).wait_recv()

    def modulation():
        prev = jnp.maximum(section - 1, 0)
        came = sum(
            jnp.where(target[prev * slots + j] == section, timestep[prev * slots + j], 0)
            for j in range(slots)
        )
        step0, step1 = timestep[section * slots], timestep[section * slots + 1]
        step_a = jnp.where(flags[0] != 0, step0, step1)
        step_b = jnp.where(flags[0] != 0, step1, step0)
        half_width = FREQ // 2
        row = lax.broadcasted_iota(jnp.int32, (8, half_width), 0)
        steps = jnp.where(row == 0, step_a, jnp.where(row == 1, step_b, came)).astype(F32)
        lane = lax.broadcasted_iota(jnp.int32, (8, half_width), 1).astype(F32)
        angles = steps * jnp.exp(-math.log(10000.0) * lane / half_width)
        embed = jnp.concatenate([jnp.cos(angles), jnp.sin(angles)], axis=1)
        rest = embed / (1.0 + jnp.exp(-embed))
        terms = []
        for _ in range(3):
            terms.append(rest.astype(BF16).astype(F32))
            rest = rest - terms[-1]
        terms = jnp.concatenate(terms, axis=0).astype(BF16)
        load_mod.wait()
        for part in range(3):
            sums = jnp.dot(terms, w_mod[part], preferred_element_type=F32)
            mods[part] = sums[0:8] + sums[8:16] + sums[16:24]
        quarter = width // 4
        for part in range(2):
            for q in range(4):
                mods_out[part * 4 + q : part * 4 + q + 1, :] = mods[
                    part, 2:3, q * quarter : (q + 1) * quarter
                ]

        @pl.when(has_prev)
        def _():
            mods_copy().start()

    def unpack():
        for i in range(tok // 16):
            rows = slice(i * 16, (i + 1) * 16)
            both = pltpu.einshape("asc->sac", latents[rows])
            pick = mask(flags[0], (16, width))
            raw[0, rows, :] = jnp.where(pick, both[0], both[1])
            raw[1, rows, :] = jnp.where(pick, both[1], both[0])

    def norm(slot):
        shift = mods[0, slot : slot + 1, :]
        scale = mods[1, slot : slot + 1, :]
        if slot == 0:
            moved = mask(any_move, shift.shape)
            came = [
                jnp.concatenate([mods_in[4 * part + q : 4 * part + q + 1, :] for q in range(4)], axis=1)
                for part in range(2)
            ]
            shift = jnp.where(moved, came[0], shift)
            scale = jnp.where(moved, came[1], scale)
        scale = 1.0 + scale

        def rows16(i, _):
            rows = pl.ds(pl.multiple_of(i * 16, 16), 16)
            values = raw[slot, rows, :].astype(F32)
            centred = values - jnp.mean(values, axis=-1, keepdims=True)
            variance = jnp.mean(centred * centred, axis=-1, keepdims=True)
            gathered[slot, me, rows, :] = (
                centred * lax.rsqrt(variance + 1e-06) * scale + shift
            ).astype(BF16)
            return 0

        lax.fori_loop(0, tok // 16, rows16, 0)

    def begin(n, *kinds):
        for kind in kinds:
            send(n, kind).start()

    def forward_x(n):
        arrive(n, 0)
        send(n, 3).start()
        send(n, 5).start()
        send(n, 4).start()
        if n == 0:
            hand(1)

    def forward_y(n):
        arrive(n, 1)
        arrive(n, 9)
        send(n, 6).start()
        if n == 0:
            hand(2)

    def last_forward(n):
        arrive(n, 3)
        send(n, 7).start()
        if n == 0:
            hand(3)
        arrive(n, 5)
        send(n, 8).start()
        if n == 0:
            hand(4)

    mix_targets = [dev_x, dev_x + to_c, dev_c]

    def mix_copy(slot, k, owner):
        return pltpu.make_async_remote_copy(
            mix_send.at[slot, mix_targets[k] % 4],
            mix_recv.at[slot, :, pl.ds(pl.multiple_of(owner % 4 * local, local), local)],
            mix_sem.at[0, slot, k], mix_sem.at[1, slot, k],
            device_id=(section, mix_targets[k]), device_id_type=MESH,
        )

    def project(slot, first, end):
        def step(k, _):
            chip = (y + k // 2) % 2 * 2 + (x + k % 2) % 2
            hidden = gathered[slot, pl.ds(2 * chip, 2)].reshape(2 * tok, width)
            rows = pl.ds(pl.multiple_of(chip * 2 * tok, 2 * tok), 2 * tok)
            for part in range(3):
                qkv[slot, rows, part * local : (part + 1) * local] = jnp.dot(
                    hidden, w_qkv[part], preferred_element_type=F32
                ).astype(BF16)
            return 0

        lax.fori_loop(first, end, step, 0)

    def queries(slot, first, end):
        def step(k, _):
            chip_x = (x + 1 + k // 2) % 2
            chip_y = k % 2
            rows = pl.ds(pl.multiple_of((chip_y * 2 + chip_x) * 2 * tok, 2 * tok), 2 * tok)
            for h in range(heads):
                a = h * HEAD_DIM
                query = qkv[slot, rows, a : a + HEAD_DIM]
                keys = qkv[slot, :, local + a : local + a + HEAD_DIM]
                vals = qkv[slot, :, 2 * local + a : 2 * local + a + HEAD_DIM]
                scores = lax.dot_general(
                    query, keys, (((1,), (1,)), ((), ())), preferred_element_type=F32
                )
                top = jnp.max(scores, axis=-1, keepdims=True)
                probs = jnp.exp((scores - top) * HEAD_DIM ** (-0.5))
                total = jnp.sum(probs, axis=-1, keepdims=True)
                mixed = jnp.dot(probs.astype(BF16), vals, preferred_element_type=F32) / total
                mixed = mixed.astype(BF16).reshape(2, tok, HEAD_DIM)
                at = pl.ds(pl.multiple_of(chip_y * tok, tok), tok)
                mix_send[slot, pl.ds(2 * chip_x, 2), at, a : a + HEAD_DIM] = mixed
            return 0

        lax.fori_loop(first, end, step, 0)

    def mix(slot, *ks):
        for k in ks:
            mix_copy(slot, k, me).start()
        if 2 in ks:
            mix_recv[slot, :, pl.ds(pl.multiple_of(row * local, local), local)] = mix_send[slot, row]

    def mix_arrive(slot):
        for k in range(3):
            mix_copy(slot, k, mix_targets[k]).wait_recv()

    def part_copy(slot, j):
        return pltpu.make_async_remote_copy(
            part_send.at[slot, j], part_recv.at[slot, j],
            part_sem.at[0, slot, j], part_sem.at[1, slot, j],
            device_id=(section, dev_y), device_id_type=MESH,
        )

    def project_out(slot, j):
        table = w_out[j].reshape(4 * local, cols)
        theirs = mix_recv[slot, pl.ds(pl.multiple_of((1 - y) * tok, tok), tok), :]
        part_send[slot, j] = jnp.dot(theirs, table, preferred_element_type=F32).astype(BF16)
        part_copy(slot, j).start()
        ours = mix_recv[slot, pl.ds(pl.multiple_of(y * tok, tok), tok), :]
        part[slot, j] = jnp.dot(ours, table, preferred_element_type=F32)

    def combine(slot, j):
        part_copy(slot, j).wait_recv()
        at = slice(j * cols, (j + 1) * cols)
        proj = part[slot, j] + part_recv[slot, j].astype(F32)
        change = mods[2, slot : slot + 1, at] * proj
        if slot == 2:
            back[j] = change.astype(BF16)

            @pl.when(has_prev)
            def _():
                back_copy(j).start()

            return
        hold[slot, j] = (raw[slot, :, at].astype(F32) + change).astype(BF16)

    def store_copy(j):
        at = slice(j * cols, (j + 1) * cols)
        return pltpu.make_async_copy(
            updated.at[:, :, at], updated_hbm.at[:, :, at], store_sem.at[j]
        )

    def write(j):
        @pl.when(has_next)
        def _():
            back_copy(j).wait_recv()

        at = slice(j * cols, (j + 1) * cols)
        pick = mask(flags[0], (16, cols))
        moved = mask(any_move, (16, cols))
        for i in range(tok // 16):
            rows = slice(i * 16, (i + 1) * 16)
            returned = raw[0, rows, at].astype(F32) + back_in[j, rows, :].astype(F32)
            first = jnp.where(moved, returned.astype(BF16), hold[0, j, rows, :])
            second = hold[1, j, rows, :]
            updated[rows, 0, at] = jnp.where(pick, first, second)
            updated[rows, 1, at] = jnp.where(pick, second, first)
        store_copy(j).start()

    everything = range(CHUNKS)
    early, late = everything[: CHUNKS // 2], everything[CHUNKS // 2 :]
    table_begin(0)
    modulation()
    load_latents.wait()
    unpack()
    norm(1)
    begin(1, 1, 2)

    @pl.when(has_next)
    def _():
        mods_copy().wait_recv()

    norm(0)
    begin(0, 0, 1, 9, 2)
    hand(0)
    begin(1, 0)
    table_begin(*early[1:])
    load_qkv.wait()
    arrive(0, 2)
    project(0, 0, 1)
    arrive(1, 2)
    project(1, 0, 1)
    forward_x(0)
    forward_y(0)
    begin(1, 9)
    for kind in (4, 6):
        arrive(0, kind)
    project(0, 1, 3)
    share(0)
    forward_x(1)
    last_forward(0)
    for kind in (7, 8):
        arrive(0, kind)
    project(0, 3, 4)
    queries(0, 0, 2)
    mix(0, 0, 1)
    table_begin(*late)
    share(1)
    table_forward(*early[: len(early) // 2])
    queries(0, 2, 4)
    mix(0, 2)
    shared(0, 1)
    project(2, 0, 2)
    table_forward(*early[len(early) // 2 :])
    forward_y(1)
    share(2)
    arrive(1, 4)
    arrive(1, 6)
    project(1, 1, 3)
    mix_arrive(0)
    for j in early:
        table_arrive(j)
        project_out(0, j)
    table_forward(*late[: len(late) // 2])
    last_forward(1)
    share(3, 4)
    for kind in (7, 8):
        arrive(1, kind)
    project(1, 3, 4)
    shared(2, 3, 4)
    project(2, 2, 4)
    queries(2, 0, 2)
    mix(2, 0, 1)
    table_forward(*late[len(late) // 2 :])
    for j in late:
        table_arrive(j)
        project_out(0, j)
    queries(2, 2, 4)
    mix(2, 2)
    queries(1, 0, 2)
    mix(1, 0, 1)
    mix_arrive(2)
    for j in everything:
        project_out(2, j)
    queries(1, 2, 4)
    mix(1, 2)
    for j in everything:
        combine(0, j)
    mix_arrive(1)
    for j in everything:
        project_out(1, j)
    for j in everything:
        combine(2, j)
    for j in everything:
        combine(1, j)
    for j in everything:
        write(j)
    for j in range(CHUNKS):
        store_copy(j).wait()

        @pl.when(has_prev)
        def _():
            back_copy(j).wait_send()

    @pl.when(has_next)
    def _():
        for k in range(len(handed)):
            hand_copy(k).wait_send()

    @pl.when(has_prev)
    def _():
        mods_copy().wait_send()
        for k in range(len(handed)):
            share_copy(k, 0).wait_send()

    for n in range(slots):
        for kind in range(len(comes)):
            send(n, kind).wait_send()
    for j in everything:
        for kind in range(3):
            table_copy(j, kind, 0).wait_send()
    for slot in range(slots + 1):
        for k in range(3):
            mix_copy(slot, k, me).wait_send()
        for j in everything:
            part_copy(slot, j).wait_send()


def kernel_body(sections, latents, timestep, target, qkv_weight, mod_weight, out_weight):
    tok, slots, width = latents.shape
    local = out_weight.shape[1]
    peers = width // local
    smem = pl.BlockSpec(memory_space=pltpu.SMEM)
    hbm = pl.BlockSpec(memory_space=pl.ANY)
    cols = width // CHUNKS
    dma = pltpu.SemaphoreType.DMA
    updated = pl.pallas_call(
        functools.partial(block_kernel, sections),
        out_shape=jax.ShapeDtypeStruct((tok, slots, width), BF16),
        in_specs=[smem, smem, hbm, hbm, hbm, hbm],
        out_specs=hbm,
        scratch_shapes=[
            pltpu.VMEM((tok, slots, width), BF16),
            pltpu.VMEM((slots, tok, width), BF16),
            pltpu.VMEM((3, FREQ, width), BF16),
            pltpu.VMEM((3, 8, width), F32),
            pltpu.VMEM((8, width // 4), F32),
            pltpu.VMEM((8, width // 4), F32),
            pltpu.VMEM((slots + 1, peers, tok, width), BF16),
            pltpu.VMEM((CHUNKS, 4, local, cols), BF16),
            pltpu.VMEM((3, width, local), BF16),
            pltpu.VMEM((slots + 1, peers * tok, 3 * local), BF16),
            pltpu.VMEM((slots + 1, 4, 2 * tok, local), BF16),
            pltpu.VMEM((slots + 1, 2 * tok, 4 * local), BF16),
            pltpu.VMEM((slots + 1, CHUNKS, tok, cols), F32),
            pltpu.VMEM((slots + 1, CHUNKS, tok, cols), BF16),
            pltpu.VMEM((slots + 1, CHUNKS, tok, cols), BF16),
            pltpu.VMEM((CHUNKS, tok, cols), BF16),
            pltpu.VMEM((CHUNKS, tok, cols), BF16),
            pltpu.VMEM((slots, CHUNKS, tok, cols), BF16),
            pltpu.VMEM((tok, slots, width), BF16),
            dma((CHUNKS + 3,)),
            dma((slots, 10)),
            dma((slots, 10)),
            dma((2, CHUNKS, 3)),
            dma((2, slots + 1, 3)),
            dma((2, slots + 1, CHUNKS)),
            dma((2, 5)),
            dma((2, 5)),
            dma((2,)),
            dma((2, CHUNKS)),
            dma((CHUNKS,)),
        ],
        compiler_params=pltpu.CompilerParams(
            collective_id=0, has_side_effects=True, vmem_limit_bytes=60 * 1024 * 1024
        ),
    )(
        target,
        timestep,
        latents,
        jnp.transpose(mod_weight[0], (1, 0, 2)),
        jnp.transpose(qkv_weight[0], (1, 0, 2)),
        out_weight[0],
    )
    return updated


def solution(mesh):
    sections = mesh.shape["section"]
    plan = functools.partial(kernel_body, sections) if mesh.shape["tp"] == 8 else body

    return jax.shard_map(
        plan,
        mesh=mesh,
        in_specs=(
            P("tp", "section", None),
            P(),
            P(),
            P("section", None, None, "tp"),
            P("section", None, None, None),
            P("section", "tp", None),
        ),
        out_specs=P("tp", "section", None),
        check_vma=False,
    )
```

```python
import functools
import math

import jax
import jax.numpy as jnp
from jax import lax
from jax.experimental import pallas as pl
from jax.experimental.pallas import tpu as pltpu
from jax.sharding import PartitionSpec as P

HEAD_DIM = 128
FREQ = 256
MOVE_MAX = 1


def from_behind(shard, axis, by):
    peers = lax.axis_size(axis)
    pairs = [(i, i + by) for i in range(peers) if 0 <= i + by < peers]
    return lax.ppermute(shard, axis, pairs)


def time_embed(steps):
    half_width = FREQ // 2
    frequency = jnp.exp(-math.log(10000.0) * jnp.arange(half_width, dtype=jnp.float32) / half_width)
    angles = steps.astype(jnp.float32)[:, None] * frequency[None, :]
    return jnp.concatenate([jnp.cos(angles), jnp.sin(angles)], axis=1)


def modulate(steps, mod_table):
    feature = jax.nn.silu(time_embed(steps))
    return jnp.einsum(
        "bf,fcd->bcd", feature, mod_table.astype(jnp.float32), precision=lax.Precision.HIGHEST
    )


def normalize(values, shift, scale):
    row_mean = jnp.mean(values, axis=-1, keepdims=True)
    centred = values - row_mean
    variance = jnp.mean(centred * centred, axis=-1, keepdims=True)
    return centred * lax.rsqrt(variance + 1e-06) * (1.0 + scale) + shift


def expert_block(batch, steps, qkv_local, mod_table, out_local):
    mods = modulate(steps, mod_table)
    values = batch.astype(jnp.float32)
    hidden = normalize(values, mods[None, :, 0], mods[None, :, 1]).astype(jnp.bfloat16)
    packed = jnp.einsum(
        "sbd,dce->sbce",
        lax.all_gather(hidden, "tp", axis=0, tiled=True),
        qkv_local,
        preferred_element_type=jnp.float32,
    ).astype(jnp.bfloat16)
    tok_all = packed.shape[0]
    slot_count = packed.shape[1]
    local_width = packed.shape[3]
    head_local = local_width // HEAD_DIM
    split_heads = packed.reshape(tok_all, slot_count, 3, head_local, HEAD_DIM)
    query = split_heads[:, :, 0]
    keys_now = split_heads[:, :, 1]
    vals_now = split_heads[:, :, 2]
    scores = jnp.einsum(
        "qbhe,kbhe->bhqk", query, keys_now, preferred_element_type=jnp.float32
    ) * HEAD_DIM ** (-0.5)
    soft = jax.nn.softmax(scores, axis=-1).astype(jnp.bfloat16)
    mixed = jnp.einsum("bhqk,kbhe->qbhe", soft, vals_now, preferred_element_type=jnp.float32)
    mixed = mixed.astype(jnp.bfloat16).reshape(tok_all, slot_count, local_width)
    proj = lax.psum_scatter(
        jnp.einsum("sbk,kd->sbd", mixed, out_local, preferred_element_type=jnp.float32).astype(
            jnp.bfloat16
        ),
        "tp",
        scatter_dimension=0,
        tiled=True,
    ).astype(jnp.float32)
    return (values + mods[None, :, 2] * proj).astype(jnp.bfloat16)


def movers_first(move_flags, slots):
    order_keys = jnp.where(move_flags, 0, 1).astype(jnp.int32) * slots + jnp.arange(
        slots, dtype=jnp.int32
    )
    return jnp.argsort(order_keys)[:MOVE_MAX]


def body(latents, timestep, target, qkv_weight, mod_weight, out_weight):
    slots = latents.shape[1]
    home_section = lax.axis_index("section")
    prev_section = jnp.maximum(home_section - 1, 0)
    own_steps = lax.dynamic_slice_in_dim(timestep, home_section * slots, slots)
    own_target = lax.dynamic_slice_in_dim(target, home_section * slots, slots)
    prev_steps = lax.dynamic_slice_in_dim(timestep, prev_section * slots, slots)
    prev_target = lax.dynamic_slice_in_dim(target, prev_section * slots, slots)
    own_move = own_target != home_section
    prev_move = prev_target == home_section
    qkv_local = qkv_weight[0]
    mod_table = mod_weight[0]
    out_local = out_weight[0]
    own_order = movers_first(own_move, slots)
    prev_order = movers_first(prev_move, slots)
    outgoing = jnp.take(latents, own_order, axis=1)
    incoming = from_behind(outgoing, "section", 1)
    batch = jnp.concatenate([latents, incoming], axis=1)
    steps = jnp.concatenate([own_steps, jnp.take(prev_steps, prev_order, axis=0)], axis=0)
    result = expert_block(batch, steps, qkv_local, mod_table, out_local)
    coming_back = from_behind(result[:, slots:], "section", -1)
    placing = own_order[None, :] == jnp.arange(slots, dtype=jnp.int32)[:, None]
    returned = jnp.einsum(
        "lm,sme->sle", placing.astype(jnp.bfloat16), coming_back, preferred_element_type=jnp.float32
    ).astype(jnp.bfloat16)
    return jnp.where(own_move[None, :, None], returned, result[:, :slots])


MESH = pl.DeviceIdType.MESH
F32 = jnp.float32
BF16 = jnp.bfloat16
CHUNKS = 4


def block_kernel(
    sections, target, timestep, latents_hbm, w_mod_hbm, w_qkv_hbm, w_out_hbm,
    updated_hbm,
    latents, raw, w_mod, mods, mods_out, mods_in, gathered, w_out, w_qkv, qkv, mix_send, mix_recv,
    part, part_send, part_recv, back, back_in, hold, updated,
    load_sem, send_sem, recv_sem, table_sem, mix_sem, part_sem, hand_sem, share_sem, mods_sem,
    back_sem, store_sem,
):
    tok, slots, width = latents.shape
    local = w_out.shape[2]
    heads = local // HEAD_DIM
    peers = gathered.shape[1]
    cols = width // CHUNKS
    section = lax.axis_index("section")
    me = lax.axis_index("tp")
    core = me % 2
    x = (me // 2) % 2
    y = me // 4
    to_x = 2 - 4 * x
    to_y = 4 - 8 * y
    to_c = 1 - 2 * core
    dev_x, dev_y, dev_c = me + to_x, me + to_y, me + to_c
    diag = me + to_x + to_y
    row = me % 4
    has_prev = section > 0
    has_next = section < sections - 1

    load_out = [
        pltpu.make_async_copy(
            w_out_hbm.at[:, j * cols : (j + 1) * cols], w_out.at[j, row], load_sem.at[j]
        )
        for j in range(CHUNKS)
    ]
    load_qkv = pltpu.make_async_copy(w_qkv_hbm, w_qkv, load_sem.at[CHUNKS])
    load_mod = pltpu.make_async_copy(w_mod_hbm, w_mod, load_sem.at[CHUNKS + 1])
    load_latents = pltpu.make_async_copy(latents_hbm, latents, load_sem.at[CHUNKS + 2])
    for copy in (load_out[0], load_latents, load_mod, *load_out[1:], load_qkv):
        copy.start()

    barrier = pltpu.get_barrier_semaphore()
    for step in range(1, peers):
        pl.semaphore_signal(
            barrier, inc=1, device_id=(section, (me + step) % peers), device_id_type=MESH
        )

    @pl.when(has_prev)
    def _():
        pl.semaphore_signal(barrier, inc=1, device_id=(section - 1, me), device_id_type=MESH)

    @pl.when(has_next)
    def _():
        pl.semaphore_signal(barrier, inc=1, device_id=(section + 1, me), device_id_type=MESH)

    beside = jnp.minimum(section, 1) + jnp.minimum(sections - 1 - section, 1)
    pl.semaphore_wait(barrier, peers - 1 + beside)

    def mods_copy():
        return pltpu.make_async_remote_copy(
            mods_out, mods_in, mods_sem.at[0], mods_sem.at[1],
            device_id=(section - 1, me), device_id_type=MESH,
        )

    def back_copy(j):
        return pltpu.make_async_remote_copy(
            back.at[j], back_in.at[j], back_sem.at[0, j], back_sem.at[1, j],
            device_id=(section - 1, me), device_id_type=MESH,
        )

    flags = [(target[section * slots + j] != section).astype(jnp.int32) for j in range(slots)]
    any_move = jnp.maximum(flags[0], flags[1])

    def mask(flag, shape):
        return jnp.broadcast_to(flag, shape) != 0

    def piece(slot, owner, part):
        rows = gathered.shape[2]
        if part is None:
            return gathered.at[slot, owner]
        return gathered.at[slot, owner, pl.ds(part * (rows // 2), rows // 2)]

    comes = [
        dev_x, dev_y, dev_c, diag, dev_x + to_c, diag, dev_y + to_c, diag + to_c, diag + to_c,
        dev_y,
    ]

    def route(n, kind):
        return [
            (me, None, dev_x), (me, 0, dev_y), (me, None, dev_c),
            (dev_x, 0, dev_y), (dev_x, None, dev_c),
            (dev_x, 1, dev_y), (dev_y, None, dev_c),
            (diag, 0, dev_c), (diag, 1, dev_c), (me, 1, dev_y),
        ][kind]

    def send(n, kind):
        owner, part, target = route(n, kind)
        ref = piece(n, owner, part)
        return pltpu.make_async_remote_copy(
            ref, ref, send_sem.at[n, kind], recv_sem.at[n, kind],
            device_id=(section, target), device_id_type=MESH,
        )

    def arrive(n, kind):
        _, part, target = route(n, kind)
        ref = piece(n, comes[kind], part)
        pltpu.make_async_remote_copy(
            ref, ref, send_sem.at[n, kind], recv_sem.at[n, kind],
            device_id=(section, target), device_id_type=MESH,
        ).wait_recv()

    def table_copy(j, kind, shift):
        owner, target = [(me, dev_x), (me, dev_c), (dev_x, dev_c)][kind]
        ref = w_out.at[j, (owner + shift) % 4]
        return pltpu.make_async_remote_copy(
            ref, ref, table_sem.at[0, j, kind], table_sem.at[1, j, kind],
            device_id=(section, target), device_id_type=MESH,
        )

    def table_begin(*js):
        for j in js:
            load_out[j].wait()
            table_copy(j, 0, 0).start()
            table_copy(j, 1, 0).start()

    def table_forward(*js):
        for j in js:
            table_copy(j, 0, to_x).wait_recv()
            table_copy(j, 2, 0).start()

    def table_arrive(*js):
        for j in js:
            table_copy(j, 1, to_c).wait_recv()
            table_copy(j, 2, to_c).wait_recv()

    handed = [(me, None), (dev_x, None), (dev_y, None), (diag, 0), (diag, 1)]

    def hand_copy(k):
        owner, part = handed[k]
        return pltpu.make_async_remote_copy(
            piece(0, owner, part), piece(2, owner, part),
            hand_sem.at[0, k], hand_sem.at[1, k],
            device_id=(section + 1, me), device_id_type=MESH,
        )

    def hand(k):
        @pl.when(has_next)
        def _():
            hand_copy(k).start()

    def share_copy(k, shift):
        owner, part = handed[k]
        ref = piece(2, owner + shift, part)
        return pltpu.make_async_remote_copy(
            ref, ref, share_sem.at[0, k], share_sem.at[1, k],
            device_id=(section, dev_c), device_id_type=MESH,
        )

    def share(*ks):
        @pl.when(has_prev)
        def _():
            for k in ks:
                hand_copy(k).wait_recv()
                share_copy(k, 0).start()

    def shared(*ks):
        @pl.when(has_prev)
        def _():
            for k in ks:
                share_copy(k, to_c).wait_recv()

    def modulation():
        prev = jnp.maximum(section - 1, 0)
        came = sum(
            jnp.where(target[prev * slots + j] == section, timestep[prev * slots + j], 0)
            for j in range(slots)
        )
        step0, step1 = timestep[section * slots], timestep[section * slots + 1]
        step_a = jnp.where(flags[0] != 0, step0, step1)
        step_b = jnp.where(flags[0] != 0, step1, step0)
        half_width = FREQ // 2
        row = lax.broadcasted_iota(jnp.int32, (8, half_width), 0)
        steps = jnp.where(row == 0, step_a, jnp.where(row == 1, step_b, came)).astype(F32)
        lane = lax.broadcasted_iota(jnp.int32, (8, half_width), 1).astype(F32)
        angles = steps * jnp.exp(-math.log(10000.0) * lane / half_width)
        embed = jnp.concatenate([jnp.cos(angles), jnp.sin(angles)], axis=1)
        rest = embed / (1.0 + jnp.exp(-embed))
        terms = []
        for _ in range(3):
            terms.append(rest.astype(BF16).astype(F32))
            rest = rest - terms[-1]
        terms = jnp.concatenate(terms, axis=0).astype(BF16)
        load_mod.wait()
        for part in range(3):
            sums = jnp.dot(terms, w_mod[part], preferred_element_type=F32)
            mods[part] = sums[0:8] + sums[8:16] + sums[16:24]
        quarter = width // 4
        for part in range(2):
            for q in range(4):
                mods_out[part * 4 + q : part * 4 + q + 1, :] = mods[
                    part, 2:3, q * quarter : (q + 1) * quarter
                ]

        @pl.when(has_prev)
        def _():
            mods_copy().start()

    def unpack():
        for i in range(tok // 16):
            rows = slice(i * 16, (i + 1) * 16)
            both = pltpu.einshape("asc->sac", latents[rows])
            pick = mask(flags[0], (16, width))
            raw[0, rows, :] = jnp.where(pick, both[0], both[1])
            raw[1, rows, :] = jnp.where(pick, both[1], both[0])

    def norm(slot):
        shift = mods[0, slot : slot + 1, :]
        scale = mods[1, slot : slot + 1, :]
        if slot == 0:
            moved = mask(any_move, shift.shape)
            came = [
                jnp.concatenate([mods_in[4 * part + q : 4 * part + q + 1, :] for q in range(4)], axis=1)
                for part in range(2)
            ]
            shift = jnp.where(moved, came[0], shift)
            scale = jnp.where(moved, came[1], scale)
        scale = 1.0 + scale

        def rows16(i, _):
            rows = pl.ds(pl.multiple_of(i * 16, 16), 16)
            values = raw[slot, rows, :].astype(F32)
            centred = values - jnp.mean(values, axis=-1, keepdims=True)
            variance = jnp.mean(centred * centred, axis=-1, keepdims=True)
            gathered[slot, me, rows, :] = (
                centred * lax.rsqrt(variance + 1e-06) * scale + shift
            ).astype(BF16)
            return 0

        lax.fori_loop(0, tok // 16, rows16, 0)

    def begin(n, *kinds):
        for kind in kinds:
            send(n, kind).start()

    def forward_x(n):
        arrive(n, 0)
        send(n, 3).start()
        send(n, 5).start()
        send(n, 4).start()
        if n == 0:
            hand(1)

    def forward_y(n):
        arrive(n, 1)
        arrive(n, 9)
        send(n, 6).start()
        if n == 0:
            hand(2)

    def last_forward(n):
        arrive(n, 3)
        send(n, 7).start()
        if n == 0:
            hand(3)
        arrive(n, 5)
        send(n, 8).start()
        if n == 0:
            hand(4)

    mix_targets = [dev_x, dev_x + to_c, dev_c]

    def mix_copy(slot, k, owner):
        return pltpu.make_async_remote_copy(
            mix_send.at[slot, mix_targets[k] % 4],
            mix_recv.at[slot, :, pl.ds(pl.multiple_of(owner % 4 * local, local), local)],
            mix_sem.at[0, slot, k], mix_sem.at[1, slot, k],
            device_id=(section, mix_targets[k]), device_id_type=MESH,
        )

    def project(slot, first, end):
        def step(k, _):
            chip = (y + k // 2) % 2 * 2 + (x + k % 2) % 2
            hidden = gathered[slot, pl.ds(2 * chip, 2)].reshape(2 * tok, width)
            rows = pl.ds(pl.multiple_of(chip * 2 * tok, 2 * tok), 2 * tok)
            for part in range(3):
                qkv[slot, rows, part * local : (part + 1) * local] = jnp.dot(
                    hidden, w_qkv[part], preferred_element_type=F32
                ).astype(BF16)
            return 0

        lax.fori_loop(first, end, step, 0)

    def queries(slot, first, end):
        def step(k, _):
            chip_x = (x + 1 + k // 2) % 2
            chip_y = k % 2
            rows = pl.ds(pl.multiple_of((chip_y * 2 + chip_x) * 2 * tok, 2 * tok), 2 * tok)
            for h in range(heads):
                a = h * HEAD_DIM
                query = qkv[slot, rows, a : a + HEAD_DIM]
                keys = qkv[slot, :, local + a : local + a + HEAD_DIM]
                vals = qkv[slot, :, 2 * local + a : 2 * local + a + HEAD_DIM]
                scores = lax.dot_general(
                    query, keys, (((1,), (1,)), ((), ())), preferred_element_type=F32
                )
                top = jnp.max(scores, axis=-1, keepdims=True)
                probs = jnp.exp((scores - top) * HEAD_DIM ** (-0.5))
                total = jnp.sum(probs, axis=-1, keepdims=True)
                mixed = jnp.dot(probs.astype(BF16), vals, preferred_element_type=F32) / total
                mixed = mixed.astype(BF16).reshape(2, tok, HEAD_DIM)
                at = pl.ds(pl.multiple_of(chip_y * tok, tok), tok)
                mix_send[slot, pl.ds(2 * chip_x, 2), at, a : a + HEAD_DIM] = mixed
            return 0

        lax.fori_loop(first, end, step, 0)

    def mix(slot, *ks):
        for k in ks:
            mix_copy(slot, k, me).start()
        if 2 in ks:
            mix_recv[slot, :, pl.ds(pl.multiple_of(row * local, local), local)] = mix_send[slot, row]

    def mix_arrive(slot):
        for k in range(3):
            mix_copy(slot, k, mix_targets[k]).wait_recv()

    def part_copy(slot, j):
        return pltpu.make_async_remote_copy(
            part_send.at[slot, j], part_recv.at[slot, j],
            part_sem.at[0, slot, j], part_sem.at[1, slot, j],
            device_id=(section, dev_y), device_id_type=MESH,
        )

    def project_out(slot, j):
        table = w_out[j].reshape(4 * local, cols)
        theirs = mix_recv[slot, pl.ds(pl.multiple_of((1 - y) * tok, tok), tok), :]
        part_send[slot, j] = jnp.dot(theirs, table, preferred_element_type=F32).astype(BF16)
        part_copy(slot, j).start()
        ours = mix_recv[slot, pl.ds(pl.multiple_of(y * tok, tok), tok), :]
        part[slot, j] = jnp.dot(ours, table, preferred_element_type=F32)

    def combine(slot, j):
        part_copy(slot, j).wait_recv()
        at = slice(j * cols, (j + 1) * cols)
        proj = part[slot, j] + part_recv[slot, j].astype(F32)
        change = mods[2, slot : slot + 1, at] * proj
        if slot == 2:
            back[j] = change.astype(BF16)

            @pl.when(has_prev)
            def _():
                back_copy(j).start()

            return
        hold[slot, j] = (raw[slot, :, at].astype(F32) + change).astype(BF16)

    def store_copy(slot, j):
        at = slice(slot * width + j * cols, slot * width + (j + 1) * cols)
        return pltpu.make_async_copy(updated.at[:, at], updated_hbm.at[:, at], store_sem.at[slot, j])

    def write(j):
        @pl.when(has_next)
        def _():
            back_copy(j).wait_recv()

        at = slice(j * cols, (j + 1) * cols)
        pick = mask(flags[0], (16, cols))
        moved = mask(any_move, (16, cols))
        for i in range(tok // 16):
            rows = slice(i * 16, (i + 1) * 16)
            returned = raw[0, rows, at].astype(F32) + back_in[j, rows, :].astype(F32)
            first = jnp.where(moved, returned.astype(BF16), hold[0, j, rows, :])
            second = hold[1, j, rows, :]
            updated[rows, at] = jnp.where(pick, first, second)
            updated[rows, slice(width + at.start, width + at.stop)] = jnp.where(
                pick, second, first
            )
        for slot in range(slots):
            store_copy(slot, j).start()

    everything = range(CHUNKS)
    early, late = everything[: CHUNKS // 2], everything[CHUNKS // 2 :]
    table_begin(0)
    modulation()
    load_latents.wait()
    unpack()
    norm(1)
    begin(1, 1, 2)

    @pl.when(has_next)
    def _():
        mods_copy().wait_recv()

    norm(0)
    begin(0, 0, 1, 9, 2)
    hand(0)
    begin(1, 0)
    table_begin(*early[1:])
    load_qkv.wait()
    arrive(0, 2)
    project(0, 0, 1)
    arrive(1, 2)
    project(1, 0, 1)
    forward_x(0)
    forward_y(0)
    begin(1, 9)
    for kind in (4, 6):
        arrive(0, kind)
    project(0, 1, 3)
    share(0)
    forward_x(1)
    last_forward(0)
    for kind in (7, 8):
        arrive(0, kind)
    project(0, 3, 4)
    queries(0, 0, 2)
    mix(0, 0, 1)
    table_begin(*late)
    share(1)
    table_forward(*early[: len(early) // 2])
    queries(0, 2, 4)
    mix(0, 2)
    shared(0, 1)
    project(2, 0, 2)
    table_forward(*early[len(early) // 2 :])
    forward_y(1)
    share(2)
    arrive(1, 4)
    arrive(1, 6)
    project(1, 1, 3)
    mix_arrive(0)
    for j in early:
        table_arrive(j)
        project_out(0, j)
    last_forward(1)
    table_forward(2)
    share(3, 4)
    shared(2, 3, 4)
    project(2, 2, 4)
    queries(2, 0, 2)
    mix(2, 0, 1)
    for j in (2,):
        table_arrive(j)
        project_out(0, j)
    table_forward(3)
    queries(2, 2, 4)
    mix(2, 2)
    for kind in (7, 8):
        arrive(1, kind)
    project(1, 3, 4)
    for j in (3,):
        table_arrive(j)
        project_out(0, j)
    queries(1, 0, 2)
    mix(1, 0, 1)
    mix_arrive(2)
    for j in everything:
        project_out(2, j)
    queries(1, 2, 4)
    mix(1, 2)
    for j in everything:
        combine(0, j)
    mix_arrive(1)
    for j in everything:
        project_out(1, j)
    for j in everything:
        combine(2, j)
    for j in everything:
        combine(1, j)
    for j in everything:
        write(j)
    for j in range(CHUNKS):
        for slot in range(slots):
            store_copy(slot, j).wait()

        @pl.when(has_prev)
        def _():
            back_copy(j).wait_send()

    @pl.when(has_next)
    def _():
        for k in range(len(handed)):
            hand_copy(k).wait_send()

    @pl.when(has_prev)
    def _():
        mods_copy().wait_send()
        for k in range(len(handed)):
            share_copy(k, 0).wait_send()

    for n in range(slots):
        for kind in range(len(comes)):
            send(n, kind).wait_send()
    for j in everything:
        for kind in range(3):
            table_copy(j, kind, 0).wait_send()
    for slot in range(slots + 1):
        for k in range(3):
            mix_copy(slot, k, me).wait_send()
        for j in everything:
            part_copy(slot, j).wait_send()


def spread_kernel(flat, spread):
    _, slots, width = spread.shape
    for slot in range(slots):
        spread[:, slot, :] = flat[:, slot * width : (slot + 1) * width]


def kernel_body(sections, latents, timestep, target, qkv_weight, mod_weight, out_weight):
    tok, slots, width = latents.shape
    local = out_weight.shape[1]
    peers = width // local
    smem = pl.BlockSpec(memory_space=pltpu.SMEM)
    hbm = pl.BlockSpec(memory_space=pl.ANY)
    cols = width // CHUNKS
    dma = pltpu.SemaphoreType.DMA
    updated = pl.pallas_call(
        functools.partial(block_kernel, sections),
        out_shape=jax.ShapeDtypeStruct((tok, slots * width), BF16),
        in_specs=[smem, smem, hbm, hbm, hbm, hbm],
        out_specs=hbm,
        scratch_shapes=[
            pltpu.VMEM((tok, slots, width), BF16),
            pltpu.VMEM((slots, tok, width), BF16),
            pltpu.VMEM((3, FREQ, width), BF16),
            pltpu.VMEM((3, 8, width), F32),
            pltpu.VMEM((8, width // 4), F32),
            pltpu.VMEM((8, width // 4), F32),
            pltpu.VMEM((slots + 1, peers, tok, width), BF16),
            pltpu.VMEM((CHUNKS, 4, local, cols), BF16),
            pltpu.VMEM((3, width, local), BF16),
            pltpu.VMEM((slots + 1, peers * tok, 3 * local), BF16),
            pltpu.VMEM((slots + 1, 4, 2 * tok, local), BF16),
            pltpu.VMEM((slots + 1, 2 * tok, 4 * local), BF16),
            pltpu.VMEM((slots + 1, CHUNKS, tok, cols), F32),
            pltpu.VMEM((slots + 1, CHUNKS, tok, cols), BF16),
            pltpu.VMEM((slots + 1, CHUNKS, tok, cols), BF16),
            pltpu.VMEM((CHUNKS, tok, cols), BF16),
            pltpu.VMEM((CHUNKS, tok, cols), BF16),
            pltpu.VMEM((slots, CHUNKS, tok, cols), BF16),
            pltpu.VMEM((tok, slots * width), BF16),
            dma((CHUNKS + 3,)),
            dma((slots, 10)),
            dma((slots, 10)),
            dma((2, CHUNKS, 3)),
            dma((2, slots + 1, 3)),
            dma((2, slots + 1, CHUNKS)),
            dma((2, 5)),
            dma((2, 5)),
            dma((2,)),
            dma((2, CHUNKS)),
            dma((slots, CHUNKS)),
        ],
        compiler_params=pltpu.CompilerParams(
            collective_id=0, has_side_effects=True, vmem_limit_bytes=60 * 1024 * 1024
        ),
    )(
        target,
        timestep,
        latents,
        jnp.transpose(mod_weight[0], (1, 0, 2)),
        jnp.transpose(qkv_weight[0], (1, 0, 2)),
        out_weight[0],
    )
    blocks = 1
    return pl.pallas_call(
        spread_kernel,
        grid=(blocks,),
        out_shape=jax.ShapeDtypeStruct((tok, slots, width), BF16),
        in_specs=[pl.BlockSpec((tok // blocks, slots * width), lambda i: (i, 0))],
        out_specs=pl.BlockSpec((tok // blocks, slots, width), lambda i: (i, 0, 0)),
    )(updated)


def solution(mesh):
    sections = mesh.shape["section"]
    plan = functools.partial(kernel_body, sections) if mesh.shape["tp"] == 8 else body

    return jax.shard_map(
        plan,
        mesh=mesh,
        in_specs=(
            P("tp", "section", None),
            P(),
            P(),
            P("section", None, None, "tp"),
            P("section", None, None, None),
            P("section", "tp", None),
        ),
        out_specs=P("tp", "section", None),
        check_vma=False,
    )
```
